128 devices in a mesh: mol: 4 (over y, x), pts: 32 (over z, core).
Axes of the slice: x: 2, y: 2, z: 16, core: 2. Of those that a mesh axis runs over, the one named last changes fastest.
The devices are a block of a 8x8x16 slice.
Arguments:
- points_map: bfloat16 [25600, 800], P(('mol', 'pts')), parts along dimension 0, may hold values from -0.21875 to 0.21875
- trial: bfloat16 [25600, 128], P('mol'), parts along dimension 0, may hold values from -6 to 6
- core: bfloat16 [25600, 6400], P(('mol', 'pts')), parts along dimension 0, may hold values from -2 to 4, as said below
- walkers: bfloat16 [3200, 12, 128], P('mol'), parts along dimension 0, may hold values from -6 to 6
- draws: int32 [25600, 12], P(('mol', 'pts')), parts along dimension 0, may hold values from 0 to 3
Outputs:
- new_walkers: bfloat16 [3200, 12, 128], P(('mol', 'pts')), parts along dimension 0
- energy: float32 [48], P('mol'), parts along dimension 0
The draws below stay inside these ranges and needn't reach their ends.
There are 4 independent parts, one for each index of `mol`. The reference program is written for one: setup_inputs(seed, part) draws one part's arguments, and reference() takes and returns one part's arrays. A program takes and returns all parts, laid end to end along the dimension named above; each array names one. Nothing has to cross between parts.
Inputs may be any that keep to these rules, and one draw needn't show every extreme that they name: core is symmetric.
All inputs are finite; a program needn't handle non-finite values.
Results may differ from the reference program's by a relative error of at most 0.018.
Values may be sent and summed in bfloat16 or wider, within the bound.
No kernel may reach another device: no remote copies, remote signals or barrier semaphores. Data moves between devices by JAX's collectives and lax.ppermute only.
A program may use at most 192 MiB of HBM per device.

```python
import math
import jax
import jax.numpy as jnp
from jax import lax

N = 800
NOCC = 128
POINTS = 6400
WALKERS = 12
TAYLOR = 3


def draw_core(key, part):
    first_key = jax.random.fold_in(jax.random.fold_in(key, 11), 0)
    gauss = jax.random.normal(first_key, (POINTS, POINTS), jnp.float32)
    matrix = (gauss + gauss.T) / math.sqrt(2.0 * POINTS)
    matrix = matrix + jnp.eye(POINTS, dtype=jnp.float32)
    return matrix.astype(jnp.bfloat16)


def with_ends(drawn, key, smallest, largest):
    longest = drawn.shape.index(max(drawn.shape))
    spots = []
    for shift in (0, 1):
        where = [jax.random.randint(jax.random.fold_in(key, axis), (), 0, length) for axis, length in enumerate(drawn.shape)]
        where[longest] = (where[longest] + shift) % drawn.shape[longest]
        spots.append(tuple(where))
    return drawn.at[spots[0]].set(smallest).at[spots[1]].set(largest)


def shard_levels(stream_key, extent, pieces, least, high):
    gain, own = 1.0, jax.random.fold_in(stream_key, 6)
    for position, blocks in pieces:
        steps = jnp.exp(jax.random.uniform(jax.random.fold_in(own, position), (blocks,), jnp.float32, least / len(pieces), high / len(pieces)))
        gain = gain * jnp.repeat(steps, extent[position] // blocks).reshape([-1 if axis == position else 1 for axis in range(len(extent))])
    return gain


def scatter_about(own_key, extent, scale, bound, cuts=(), kind=jnp.bfloat16):
    loudness = shard_levels(own_key, extent, cuts, -0.22, 0.18) if cuts else 1.0
    values = jax.random.normal(own_key, extent, jnp.float32) * scale * loudness
    return jnp.minimum(jnp.maximum(values, -bound), bound).astype(kind)


def setup_inputs(seed: int = 0, part: int = 0) -> dict:
    key_list = jax.random.split(jax.random.key(seed), 6)
    own_keys = jax.random.split(jax.random.fold_in(key_list[5], part), 6)
    points_map = scatter_about(own_keys[0], (POINTS, N), N ** -0.5, 0.21875, ((0, 32),))
    trial = scatter_about(own_keys[1], (POINTS, NOCC), 1.0, 6.0)
    core = draw_core(jax.random.fold_in(jax.random.fold_in(key_list[5], part), 71), part)
    walkers = scatter_about(own_keys[3], (N, WALKERS, NOCC), 1.0, 6.0)
    draws = with_ends(jax.random.randint(own_keys[4], (POINTS, WALKERS), 0, 4), jax.random.fold_in(own_keys[4], 1), 0, 3).astype(jnp.int32)
    return dict(points_map=points_map, trial=trial, core=core, walkers=walkers, draws=draws)


GAUSS_NODES = (-2.3344142, -0.7419637, 0.7419637, 2.3344142)
FIELD_STEP = 0.15

def node_lookup(draws):
    values = jnp.zeros(draws.shape, jnp.float32)
    for number, node in enumerate(GAUSS_NODES):
        values = values + jnp.where(draws == number, node, 0.0).astype(jnp.float32)
    return values

def reference(points_map, trial, core, walkers, draws):
    flat_walkers = walkers.reshape(N, WALKERS * NOCC)
    orbit = jnp.dot(points_map, flat_walkers, preferred_element_type=jnp.float32).astype(jnp.bfloat16).reshape(POINTS, WALKERS, NOCC)
    density = (lax.optimization_barrier(jnp.sum(orbit.astype(jnp.float32) * trial.astype(jnp.float32)[:, None, :], axis=2)) / math.sqrt(NOCC)).astype(jnp.bfloat16)
    potential = jnp.dot(core, density, preferred_element_type=jnp.float32)
    field = FIELD_STEP * (node_lookup(draws) - FIELD_STEP * potential)
    running = walkers.astype(jnp.float32)
    current = orbit
    term_now = walkers
    for degree in range(1, TAYLOR + 1):
        if degree > 1:
            current = jnp.dot(points_map, term_now.reshape(N, WALKERS * NOCC), preferred_element_type=jnp.float32).astype(jnp.bfloat16).reshape(POINTS, WALKERS, NOCC)
        scaled = (field[:, :, None] * current.astype(jnp.float32)).astype(jnp.bfloat16).reshape(POINTS, WALKERS * NOCC)
        summed = jnp.einsum('pi,pc->ic', points_map.astype(jnp.float32), scaled.astype(jnp.float32))
        term_now = (summed / degree).astype(jnp.bfloat16).reshape(N, WALKERS, NOCC)
        running = running + term_now.astype(jnp.float32)
    new_walkers = running.astype(jnp.bfloat16)
    hartree = lax.optimization_barrier(jnp.sum(density.astype(jnp.float32) * potential, axis=0))
    core_wide = core.astype(jnp.float32)

    def per_walker(orbit_walker):
        mixed = jnp.dot(orbit_walker, trial.T, preferred_element_type=jnp.float32)
        return jnp.sum(core_wide * mixed * mixed.T) / NOCC
    exchange = lax.map(per_walker, jnp.moveaxis(orbit, 1, 0))
    energy = (hartree - exchange) / (2.0 * POINTS)
    return (new_walkers, energy)
```

```python
import functools
import math

import jax
import jax.numpy as jnp
from jax import lax
from jax.experimental import pallas as pl
from jax.experimental.pallas import tpu as pltpu
from jax.sharding import PartitionSpec as P

TAYLOR = 3
GAUSS_NODES = (-2.3344142, -0.7419637, 0.7419637, 2.3344142)
FIELD_STEP = 0.15
BF16, F32 = jnp.bfloat16, jnp.float32
NT = (((1,), (1,)), ((), ()))
NN = (((1,), (0,)), ((), ()))
VMEM_LIMIT = 24 * 1024 * 1024


def mm(a, b, dims=NN):
    return lax.dot_general(a, b, dims, preferred_element_type=F32)


def node_lookup(draws):
    values = jnp.zeros(draws.shape, F32)
    for number, node in enumerate(GAUSS_NODES):
        values = values + jnp.where(draws == number, node, 0.0).astype(F32)
    return values


def vmem():
    return pl.BlockSpec(memory_space=pltpu.VMEM)


def cost(flops, moved):
    return pl.CostEstimate(flops=int(flops), bytes_accessed=int(moved), transcendentals=0)


def params():
    return pltpu.CompilerParams(vmem_limit_bytes=VMEM_LIMIT)


def smem():
    return pl.BlockSpec(memory_space=pltpu.SMEM)


def orbit_kernel(occupied, where_ref, own_ref, mate_ref, w_ref, trial_ref, orbit_ref, near_ref, sent_ref):
    rows = own_ref.shape[0]
    x = jnp.concatenate([own_ref[...].astype(F32), mate_ref[...].astype(F32)], axis=0).astype(BF16)
    trial = trial_ref[where_ref[0]].astype(F32)
    near = jnp.concatenate([trial, trial_ref[where_ref[1]].astype(F32)], axis=0)
    near_ref[...] = near.astype(BF16)
    lane = lax.broadcasted_iota(jnp.int32, (rows, 128), 1)
    density = jnp.zeros((rows, 128), F32)
    for pair in range(w_ref.shape[0] // (2 * occupied)):
        both = mm(x, w_ref[pair * 2 * occupied : (pair + 1) * 2 * occupied], NT).astype(BF16)
        for half in range(2):
            one = both[:, half * occupied : (half + 1) * occupied]
            walker = 2 * pair + half
            orbit_ref[walker] = one
            total = jnp.sum(one.astype(F32)[:rows] * trial, axis=1, keepdims=True)
            density = jnp.where(lane == walker, total / math.sqrt(occupied), density)
    turned = density.T[: sent_ref.shape[1]].astype(BF16)
    for device in range(sent_ref.shape[0]):
        sent_ref[device] = turned


def orbit_call(where, own, mate, turned_walkers, trial_blocks):
    rows, orbitals = own.shape
    devices, _, occupied = trial_blocks.shape
    walkers = turned_walkers.shape[0] // occupied
    return pl.pallas_call(
        functools.partial(orbit_kernel, occupied),
        out_shape=(
            jax.ShapeDtypeStruct((walkers, 2 * rows, occupied), BF16),
            jax.ShapeDtypeStruct((2 * rows, occupied), BF16),
            jax.ShapeDtypeStruct((devices, -(-walkers // 16) * 16, rows), BF16),
        ),
        in_specs=[smem()] + [vmem()] * 4,
        out_specs=(vmem(), vmem(), vmem()),
        compiler_params=params(),
        cost_estimate=cost(4 * rows * orbitals * walkers * occupied, 6e6),
        name="orbit",
    )(where, own, mate, turned_walkers, trial_blocks)


def split_kernel(where_ref, core_ref, keep_ref, away_ref):
    width = keep_ref.shape[2]
    odd = where_ref[2] == 1
    for chip in range(keep_ref.shape[0]):
        even_block = core_ref[:, 2 * chip * width : (2 * chip + 1) * width]
        odd_block = core_ref[:, (2 * chip + 1) * width : (2 * chip + 2) * width]
        keep_ref[chip] = jnp.where(odd, odd_block, even_block)
        away_ref[chip] = jnp.where(odd, even_block, odd_block)


def split_call(where, core, width):
    rows, columns = core.shape
    shape = jax.ShapeDtypeStruct((columns // width // 2, rows, width), BF16)
    return pl.pallas_call(
        split_kernel,
        out_shape=(shape, shape),
        in_specs=[smem(), vmem()],
        out_specs=(vmem(), vmem()),
        compiler_params=params(),
        cost_estimate=cost(1e6, 6e6),
        name="split",
    )(where, core)


def field_kernel(walkers, occupied, columns, where_ref, density_ref, keep_ref, away_ref, draws_ref, out_ref, hartree_ref):
    parity = where_ref[2]
    total = None
    for chip in range(keep_ref.shape[0]):
        for block, slot in ((keep_ref, parity), (away_ref, 1 - parity)):
            piece = mm(density_ref[2 * chip + slot], block[chip], NT)
            total = piece if total is None else total + piece
    mine = density_ref[where_ref[0]].astype(F32)
    hartree_ref[...] = jnp.broadcast_to(jnp.sum(mine * total, axis=1, keepdims=True), hartree_ref.shape)
    field = FIELD_STEP * (node_lookup(draws_ref[...]) - FIELD_STEP * total[:walkers])
    for chip in range(out_ref.shape[0]):
        first = columns * chip // occupied
        out_ref[chip, 0:1] = field[first : first + 1]
        second = min(first + 1, walkers - 1)
        out_ref[chip, 1:2] = field[second : second + 1]


def field_call(where, densities, keep, away, draws, occupied, columns):
    devices, padded, rows = densities.shape
    chips = keep.shape[0]
    walkers = draws.shape[0]
    return pl.pallas_call(
        functools.partial(field_kernel, walkers, occupied, columns),
        out_shape=(
            jax.ShapeDtypeStruct((chips, 2, rows), F32),
            jax.ShapeDtypeStruct((padded, 128), F32),
        ),
        in_specs=[smem()] + [vmem()] * 4,
        out_specs=(vmem(), vmem()),
        compiler_params=params(),
        cost_estimate=cost(4e9, 4e6),
        name="field",
    )(where, densities, keep, away, draws)


def exchange_kernel(
    occupied, weight, chunks, where_ref, upper_ref, lower_ref, near_ref, before_ref, w_hbm, orbit_hbm, trial_hbm,
    keep_hbm, came_hbm, out_ref, w_ref, orbit_ref, trial_ref, keep_ref, came_ref, core_ref, far_ref,
    forward_ref, backward_ref, sems,
):
    chip = where_ref[0]
    span = w_ref.shape[0] // chunks
    copies = [
        pltpu.make_async_copy(w_hbm.at[pl.ds(c * span, span)], w_ref.at[pl.ds(c * span, span)], sems.at[c])
        for c in range(chunks)
    ]
    copies += [
        pltpu.make_async_copy(keep_hbm.at[chip], keep_ref, sems.at[chunks]),
        pltpu.make_async_copy(came_hbm.at[chip], came_ref, sems.at[chunks + 1]),
        pltpu.make_async_copy(trial_hbm.at[where_ref[1]], trial_ref, sems.at[chunks + 2]),
        pltpu.make_async_copy(orbit_hbm, orbit_ref, sems.at[chunks + 3]),
    ]
    for copy in copies:
        copy.start()
    x = jnp.concatenate([upper_ref[...], lower_ref[...]], axis=0)
    rows = x.shape[0]
    for c in range(chunks):
        copies[c].wait()
        far_ref[c * span : (c + 1) * span] = mm(w_ref[c * span : (c + 1) * span], x, NT).astype(BF16)
    for copy in copies[chunks:]:
        copy.wait()
    core_ref[:rows] = keep_ref[...].astype(F32)
    core_ref[rows:] = came_ref[...].astype(F32)
    far_trial = trial_ref[...]
    walkers = out_ref.shape[0]
    forward_ref[1] = jnp.zeros(core_ref.shape, F32)
    backward_ref[1] = jnp.zeros(core_ref.shape, F32)

    def gather(walker, slot):
        value = forward_ref[slot] * backward_ref[slot] * core_ref[...]
        total = jnp.sum(value.reshape(-1, 8, rows), axis=0)
        out_ref[walker] = before_ref[walker] + weight * total

    def spread(walker, slot):
        orbit_far = far_ref[pl.ds(pl.multiple_of(walker * occupied, occupied), occupied)]
        forward_ref[slot] = mm(orbit_ref[walker], far_trial, NT)
        backward_ref[slot] = mm(near_ref[...], orbit_far)

    def two(number, carry):
        gather(lax.rem(2 * number + walkers - 1, walkers), 1)
        spread(2 * number, 0)
        gather(2 * number, 0)
        spread(2 * number + 1, 1)
        return carry

    lax.fori_loop(0, walkers // 2, two, 0)
    gather(walkers - 1, 1)


def exchange_call(where, block, turned_walkers, orbit, near, trial_blocks, keep, came, before, weight):
    walkers, near_rows, occupied = orbit.shape
    rows = keep.shape[1]
    wide, orbitals = turned_walkers.shape
    chunks = 3
    return pl.pallas_call(
        functools.partial(exchange_kernel, occupied, weight, chunks),
        out_shape=jax.ShapeDtypeStruct(before.shape, F32),
        in_specs=[smem()] + [vmem()] * 4 + [pl.BlockSpec(memory_space=pl.ANY)] * 5,
        out_specs=vmem(),
        scratch_shapes=[
            pltpu.VMEM((wide, orbitals), BF16),
            pltpu.VMEM(orbit.shape, BF16),
            pltpu.VMEM((rows, occupied), BF16),
            pltpu.VMEM((rows, rows), BF16),
            pltpu.VMEM((rows, rows), BF16),
            pltpu.VMEM((near_rows, rows), F32),
            pltpu.VMEM((wide, rows), BF16),
            pltpu.VMEM((2, near_rows, rows), F32),
            pltpu.VMEM((2, near_rows, rows), F32),
            pltpu.SemaphoreType.DMA((chunks + 4,)),
        ],
        compiler_params=params(),
        cost_estimate=cost(2 * rows * wide * (orbitals + 4 * rows), 5e6),
        name="exchange",
    )(where, *block, near, before, turned_walkers, orbit, trial_blocks, keep, came)


def energy_row(walkers, occupied, shift, partial_ref, hartree_ref, points):
    exchange = jnp.sum(jnp.sum(partial_ref[...], axis=1), axis=1, keepdims=True) / occupied
    energy = (hartree_ref[:walkers] - exchange) / (2.0 * points)
    row = lax.broadcasted_iota(jnp.int32, energy.shape, 0)
    lane = lax.broadcasted_iota(jnp.int32, energy.shape, 1)
    return jnp.sum(jnp.where(lane == row + shift, energy, 0.0), axis=0, keepdims=True)


def step_term(degree, own_ref, other_ref, running_ref):
    columns = running_ref.shape[0]
    term = ((own_ref[:columns] + other_ref[:columns]) / degree).astype(BF16)
    return term, running_ref[...] + term.astype(F32)


def degree_kernel(count, degree, occupied, where_ref, field_ref, *refs):
    blocks, refs = refs[: 2 * count], refs[2 * count :]
    refs, map_ref, sems = refs[:-2], refs[-2], refs[-1]
    copies = []
    for number in range(count):
        cut = blocks[2 * number].shape[0]
        for half, part in enumerate((pl.ds(0, cut), pl.ds(cut, map_ref.shape[1] - cut))):
            copy = pltpu.make_async_copy(
                blocks[2 * number + half], map_ref.at[number, part], sems.at[2 * number + half]
            )
            copy.start()
            copies.append(copy)
    if degree == 1:
        walkers_ref, partial_ref, hartree_ref, out_ref, running_ref = refs
        columns = walkers_ref.shape[0]
        term = walkers_ref[...]
        running_ref[...] = term.astype(F32)
        points = 2 * count * field_ref.shape[2]
        row = energy_row(partial_ref.shape[0], occupied, columns, partial_ref, hartree_ref, points)
        out_ref[columns:, :128] = jnp.broadcast_to(row, (8, 128))
    else:
        own_ref, other_ref, before_ref, out_ref, running_ref = refs
        columns = before_ref.shape[0]
        term, running = step_term(degree - 1, own_ref, other_ref, before_ref)
        running_ref[...] = running
    first = where_ref[count]
    total = None
    for number in range(count):
        copies[2 * number].wait()
        copies[2 * number + 1].wait()
        x = map_ref[number]
        current = mm(term, x, NT).astype(BF16).astype(F32)
        field = field_ref[where_ref[number]]
        column = lax.broadcasted_iota(jnp.int32, current.shape, 0)
        scaled = jnp.where(column < first, field[0:1], field[1:2]) * current
        piece = mm(scaled.astype(BF16), x)
        total = piece if total is None else total + piece
    out_ref[:columns] = total


def degree_call(where, fields, blocks, degree, occupied, columns, *rest):
    count = len(blocks)
    rows, orbitals = fields.shape[2], blocks[0][0].shape[1]
    flat = [piece for block in blocks for piece in block]
    return pl.pallas_call(
        functools.partial(degree_kernel, count, degree, occupied),
        out_shape=(
            jax.ShapeDtypeStruct((columns + 8 if degree == 1 else columns, orbitals), F32),
            jax.ShapeDtypeStruct((columns, orbitals), F32),
        ),
        in_specs=[smem(), vmem()]
        + [pl.BlockSpec(memory_space=pl.ANY)] * len(flat)
        + [vmem()] * len(rest),
        out_specs=(vmem(), vmem()),
        scratch_shapes=[
            pltpu.VMEM((count, rows, orbitals), BF16),
            pltpu.SemaphoreType.DMA((2 * count,)),
        ],
        compiler_params=params(),
        cost_estimate=cost(4 * rows * count * orbitals * columns, 6e6),
        name="degree",
    )(where, fields, *flat, *rest)


def finish_kernel(where_ref, own_ref, other_ref, before_ref, own_energy, other_energy, out_ref, turned_ref):
    columns, orbitals = before_ref.shape
    chips, own_rows, lanes = out_ref.shape
    parity = where_ref[2]
    _, running = step_term(TAYLOR, own_ref, other_ref, before_ref)
    padded = jnp.concatenate([running, jnp.zeros((lanes - columns, orbitals), F32)], axis=0)
    turned_ref[...] = padded.T
    energy = own_energy[:, :lanes] + other_energy[:, :lanes]
    top = energy.astype(BF16).astype(F32)
    middle = (energy - top).astype(BF16).astype(F32)
    low = energy - top - middle
    row = lax.broadcasted_iota(jnp.int32, (own_rows, lanes), 0)
    lane = lax.broadcasted_iota(jnp.int32, (own_rows, lanes), 1)
    extra = jnp.where(row == 0, top[0:1], jnp.where(row == 1, middle[0:1], jnp.where(row == 2, low[0:1], 0.0)))
    for chip in range(chips):
        mine = turned_ref[pl.ds((2 * chip + parity) * own_rows, own_rows)]
        out_ref[chip] = jnp.where(lane < columns, mine, extra).astype(BF16)


def finish_call(where, own, other, running, own_energy, other_energy, devices):
    columns, orbitals = running.shape
    return pl.pallas_call(
        finish_kernel,
        out_shape=jax.ShapeDtypeStruct((devices // 2, orbitals // devices, 128), BF16),
        in_specs=[smem()] + [vmem()] * 5,
        out_specs=vmem(),
        scratch_shapes=[pltpu.VMEM((orbitals, 128), F32)],
        compiler_params=params(),
        cost_estimate=cost(1e6, 2e6),
        name="finish",
    )(where, own, other, running, own_energy, other_energy)


def body(points_map, trial, core, walkers, draws):
    rows, orbitals = points_map.shape
    walker_count, occupied = walkers.shape[1:]
    devices = lax.axis_size("pts")
    chips = devices // 2
    me = lax.axis_index("pts")
    chip, parity = me // 2, me % 2
    swapped = [(i, i ^ 1) for i in range(devices)]
    forward = [(i, (i + 2) % devices) for i in range(devices)]
    backward = [(i, (i - 2) % devices) for i in range(devices)]
    same_core = [[2 * z + c for z in range(chips)] for c in range(2)]
    columns = walker_count * occupied // chips
    cut = rows // 2 // 16 * 16

    def swap(value):
        return lax.ppermute(value, "pts", swapped)

    own = (points_map[:cut], points_map[cut:])
    right, left = own, own
    blocks, offsets = [own], [0]

    def advance(right, left):
        right = tuple(lax.ppermute(piece, "pts", forward) for piece in right)
        left = tuple(lax.ppermute(piece, "pts", backward) for piece in left)
        return right, left

    mate = swap(points_map)
    place = jnp.stack([me, me ^ 1, parity]).astype(jnp.int32)
    turned = walkers.reshape(orbitals, walker_count * occupied).T
    trial_blocks = trial.reshape(devices, rows, occupied)
    orbit, near, sent = orbit_call(place, points_map, mate, turned, trial_blocks)
    densities = lax.all_to_all(sent, "pts", split_axis=0, concat_axis=0, tiled=True)
    keep, away = split_call(place, core, rows)
    came = swap(away)
    outgoing, hartree = field_call(place, densities, keep, away, draws.T, occupied, columns)
    fields = lax.all_to_all(
        outgoing, "pts", split_axis=0, concat_axis=0, tiled=True, axis_index_groups=same_core
    )

    def exchange(offset, block, before, weight):
        far = (chip + offset) % chips
        where = jnp.stack([far, 2 * far + parity]).astype(jnp.int32)
        return exchange_call(
            where, block, turned, orbit, near, trial_blocks, keep, came, before, weight
        )

    def held(pieces, partial):
        out = []
        for piece in pieces:
            piece, partial = lax.optimization_barrier((piece, partial))
            out.append(piece)
        return tuple(out), partial

    partial = jnp.zeros((walker_count, 8, rows), F32)
    half = chips // 2
    pending = (0, own, 1.0)
    for step in range(1, half):
        if step > 2:
            right, partial = held(right, partial)
            left, partial = held(left, partial)
        right, left = advance(right, left)
        partial = exchange(pending[0], pending[1], partial, pending[2])
        blocks += [right, left]
        offsets += [-step, step]
        pending = (-step, right, 2.0) if step % 2 else (step, left, 2.0)
    right, partial = held(right, partial)
    left, partial = held(left, partial)
    far_block = (lax.ppermute(right[0], "pts", forward), lax.ppermute(left[1], "pts", backward))
    partial = exchange(pending[0], pending[1], partial, pending[2])
    blocks.append(far_block)
    offsets.append(half)
    partial = exchange(half, far_block, partial, 1.0)

    start = chip * columns
    first_count = occupied - start % occupied
    sources = (chip + jnp.asarray(offsets, jnp.int32)) % chips
    where = jnp.concatenate([sources, first_count.reshape(1)]).astype(jnp.int32)
    term = lax.dynamic_slice_in_dim(turned, start, columns, 0)
    mine, running = degree_call(
        where, fields, blocks, 1, occupied, columns, term, partial, hartree
    )
    theirs = swap(mine)
    energies = (mine[columns:], theirs[columns:])
    for degree in range(2, TAYLOR + 1):
        mine, running = degree_call(
            where, fields, blocks, degree, occupied, columns, mine, theirs, running
        )
        theirs = swap(mine)
    message = finish_call(place, mine, theirs, running, *energies, devices)
    arrived = lax.all_to_all(
        message, "pts", split_axis=0, concat_axis=0, tiled=True, axis_index_groups=same_core
    )
    new_walkers = jnp.moveaxis(arrived[:, :, :columns], 0, 1)
    new_walkers = new_walkers.reshape(orbitals // devices, walker_count, occupied)
    energy = jnp.sum(arrived[:, :3, columns : columns + walker_count].astype(F32), axis=(0, 1))
    return (new_walkers, energy)


def solution(mesh):
    placed = (
        P(("mol", "pts"), None),
        P("mol", None),
        P(("mol", "pts"), None),
        P("mol", None, None),
        P(("mol", "pts"), None),
    )
    return jax.shard_map(
        body,
        mesh=mesh,
        in_specs=placed,
        out_specs=(P(("mol", "pts"), None, None), P("mol")),
        check_vma=False,
    )
```

```python
import functools
import math

import jax
import jax.numpy as jnp
from jax import lax
from jax.experimental import pallas as pl
from jax.experimental.pallas import tpu as pltpu
from jax.sharding import PartitionSpec as P

TAYLOR = 3
GAUSS_NODES = (-2.3344142, -0.7419637, 0.7419637, 2.3344142)
FIELD_STEP = 0.15
BF16, F32 = jnp.bfloat16, jnp.float32
NT = (((1,), (1,)), ((), ()))
NN = (((1,), (0,)), ((), ()))
VMEM_LIMIT = 24 * 1024 * 1024


def mm(a, b, dims=NN):
    return lax.dot_general(a, b, dims, preferred_element_type=F32)


def node_lookup(draws):
    values = jnp.zeros(draws.shape, F32)
    for number, node in enumerate(GAUSS_NODES):
        values = values + jnp.where(draws == number, node, 0.0).astype(F32)
    return values


def vmem():
    return pl.BlockSpec(memory_space=pltpu.VMEM)


def cost(flops, moved):
    return pl.CostEstimate(flops=int(flops), bytes_accessed=int(moved), transcendentals=0)


def params():
    return pltpu.CompilerParams(vmem_limit_bytes=VMEM_LIMIT)


def smem():
    return pl.BlockSpec(memory_space=pltpu.SMEM)


def orbit_kernel(occupied, where_ref, own_ref, mate_ref, w_ref, trial_any, orbit_ref, near_ref, sent_ref, trial_ref, sems):
    copies = [pltpu.make_async_copy(trial_any.at[where_ref[k]], trial_ref.at[k], sems.at[k]) for k in range(2)]
    for copy in copies:
        copy.start()
    rows = own_ref.shape[0]
    x = jnp.concatenate([own_ref[...].astype(F32), mate_ref[...].astype(F32)], axis=0).astype(BF16)
    for copy in copies:
        copy.wait()
    trial = trial_ref[0].astype(F32)
    near = jnp.concatenate([trial, trial_ref[1].astype(F32)], axis=0)
    near_ref[...] = near.astype(BF16)
    lane = lax.broadcasted_iota(jnp.int32, (rows, 128), 1)
    density = jnp.zeros((rows, 128), F32)
    for pair in range(w_ref.shape[0] // (2 * occupied)):
        both = mm(x, w_ref[pair * 2 * occupied : (pair + 1) * 2 * occupied], NT).astype(BF16)
        for half in range(2):
            one = both[:, half * occupied : (half + 1) * occupied]
            walker = 2 * pair + half
            orbit_ref[walker] = one
            total = jnp.sum(one.astype(F32)[:rows] * trial, axis=1, keepdims=True)
            density = jnp.where(lane == walker, total / math.sqrt(occupied), density)
    turned = density.T[: sent_ref.shape[1]].astype(BF16)
    for device in range(sent_ref.shape[0]):
        sent_ref[device] = turned


def orbit_call(where, own, mate, turned_walkers, trial_blocks):
    rows, orbitals = own.shape
    devices, _, occupied = trial_blocks.shape
    walkers = turned_walkers.shape[0] // occupied
    return pl.pallas_call(
        functools.partial(orbit_kernel, occupied),
        out_shape=(
            jax.ShapeDtypeStruct((walkers, 2 * rows, occupied), BF16),
            jax.ShapeDtypeStruct((2 * rows, occupied), BF16),
            jax.ShapeDtypeStruct((devices // 2, -(-walkers // 16) * 16, rows), BF16),
        ),
        in_specs=[smem()] + [vmem()] * 3 + [pl.BlockSpec(memory_space=pl.ANY)],
        out_specs=(vmem(), vmem(), vmem()),
        scratch_shapes=[pltpu.VMEM((2, rows, occupied), BF16), pltpu.SemaphoreType.DMA((2,))],
        compiler_params=params(),
        cost_estimate=cost(4 * rows * orbitals * walkers * occupied, 6e6),
        name="orbit",
    )(where, own, mate, turned_walkers, trial_blocks)


def split_kernel(where_ref, core_ref, out_ref):
    width = out_ref.shape[3]
    for block in range(core_ref.shape[1] // width):
        slot = lax.rem(block % 2 + where_ref[2], 2)
        out_ref[slot, block // 2] = core_ref[:, block * width : (block + 1) * width]


def split_call(where, core, width):
    rows, columns = core.shape
    return pl.pallas_call(
        split_kernel,
        out_shape=jax.ShapeDtypeStruct((2, columns // width // 2, rows, width), BF16),
        in_specs=[smem(), vmem()],
        out_specs=vmem(),
        compiler_params=params(),
        cost_estimate=cost(1e6, 6e6),
        name="split",
    )(where, core)


def field_kernel(walkers, occupied, columns, where_ref, mine_ref, theirs_ref, cores_ref, draws_ref, out_ref, hartree_ref):
    total = None
    for chip in range(cores_ref.shape[1]):
        for slot, density_ref in enumerate((mine_ref, theirs_ref)):
            piece = mm(density_ref[chip], cores_ref[slot, chip], NT)
            total = piece if total is None else total + piece
    mine = mine_ref[where_ref[3]].astype(F32)
    hartree_ref[...] = jnp.broadcast_to(jnp.sum(mine * total, axis=1, keepdims=True), hartree_ref.shape)
    field = FIELD_STEP * (node_lookup(draws_ref[...]) - FIELD_STEP * total[:walkers])
    for chip in range(out_ref.shape[0]):
        first = columns * chip // occupied
        out_ref[chip, 0:1] = field[first : first + 1]
        second = min(first + 1, walkers - 1)
        out_ref[chip, 1:2] = field[second : second + 1]


def field_call(where, mine, theirs, cores, draws, occupied, columns):
    chips, padded, rows = mine.shape
    walkers = draws.shape[0]
    return pl.pallas_call(
        functools.partial(field_kernel, walkers, occupied, columns),
        out_shape=(
            jax.ShapeDtypeStruct((chips, 2, rows), F32),
            jax.ShapeDtypeStruct((padded, 128), F32),
        ),
        in_specs=[smem()] + [vmem()] * 4,
        out_specs=(vmem(), vmem()),
        compiler_params=params(),
        cost_estimate=cost(4e9, 4e6),
        name="field",
    )(where, mine, theirs, cores, draws)


def exchange_kernel(
    occupied, weight, where_ref, upper_ref, lower_ref, w_ref, orbit_ref, near_ref, before_ref, trial_any, cores_any,
    came_any, out_ref, core_ref, far_ref, forward_ref, backward_ref, trial_ref, half_ref, sems,
):
    copies = [
        pltpu.make_async_copy(trial_any.at[where_ref[1]], trial_ref, sems.at[0]),
        pltpu.make_async_copy(cores_any.at[0, where_ref[0]], half_ref.at[0], sems.at[1]),
        pltpu.make_async_copy(came_any.at[0, where_ref[0]], half_ref.at[1], sems.at[2]),
    ]
    for copy in copies:
        copy.start()
    x = jnp.concatenate([upper_ref[...], lower_ref[...]], axis=0)
    rows = x.shape[0]
    far_ref[...] = mm(w_ref[...], x, NT).astype(BF16)
    for copy in copies:
        copy.wait()
    core_ref[:rows] = half_ref[0].astype(F32)
    core_ref[rows:] = half_ref[1].astype(F32)
    far_trial = trial_ref[...]
    walkers = out_ref.shape[0]
    forward_ref[1] = jnp.zeros(core_ref.shape, F32)
    backward_ref[1] = jnp.zeros(core_ref.shape, F32)

    def gather(walker, slot):
        value = forward_ref[slot] * backward_ref[slot] * core_ref[...]
        total = jnp.sum(value.reshape(-1, 8, rows), axis=0)
        out_ref[walker] = before_ref[walker] + weight * total

    def spread(walker, slot):
        orbit_far = far_ref[pl.ds(pl.multiple_of(walker * occupied, occupied), occupied)]
        forward_ref[slot] = mm(orbit_ref[walker], far_trial, NT)
        backward_ref[slot] = mm(near_ref[...], orbit_far)

    def two(number, carry):
        gather(lax.rem(2 * number + walkers - 1, walkers), 1)
        spread(2 * number, 0)
        gather(2 * number, 0)
        spread(2 * number + 1, 1)
        return carry

    lax.fori_loop(0, walkers // 2, two, 0)
    gather(walkers - 1, 1)


def exchange_call(where, block, turned_walkers, orbit, near, trial_blocks, cores, came, before, weight):
    walkers, near_rows, occupied = orbit.shape
    rows = came.shape[2]
    orbitals = turned_walkers.shape[1]
    return pl.pallas_call(
        functools.partial(exchange_kernel, occupied, weight),
        out_shape=jax.ShapeDtypeStruct(before.shape, F32),
        in_specs=[smem()] + [vmem()] * 6 + [pl.BlockSpec(memory_space=pl.ANY)] * 3,
        out_specs=vmem(),
        scratch_shapes=[
            pltpu.VMEM((near_rows, rows), F32),
            pltpu.VMEM((walkers * occupied, rows), BF16),
            pltpu.VMEM((2, near_rows, rows), F32),
            pltpu.VMEM((2, near_rows, rows), F32),
            pltpu.VMEM((rows, occupied), BF16),
            pltpu.VMEM((2, rows, rows), BF16),
            pltpu.SemaphoreType.DMA((3,)),
        ],
        compiler_params=params(),
        cost_estimate=cost(2 * rows * walkers * occupied * (orbitals + 4 * rows), 5e6),
        name="exchange",
    )(where, *block, turned_walkers, orbit, near, before, trial_blocks, cores, came)


def energy_row(walkers, occupied, shift, partial_ref, hartree_ref, points):
    exchange = jnp.sum(jnp.sum(partial_ref[...], axis=1), axis=1, keepdims=True) / occupied
    energy = (hartree_ref[:walkers] - exchange) / (2.0 * points)
    row = lax.broadcasted_iota(jnp.int32, energy.shape, 0)
    lane = lax.broadcasted_iota(jnp.int32, energy.shape, 1)
    return jnp.sum(jnp.where(lane == row + shift, energy, 0.0), axis=0, keepdims=True)


def step_term(degree, own_ref, other_ref, running_ref):
    columns = running_ref.shape[0]
    term = ((own_ref[:columns] + other_ref[:columns]) / degree).astype(BF16)
    return term, running_ref[...] + term.astype(F32)


def degree_kernel(count, degree, occupied, where_ref, field_ref, *refs):
    blocks, refs = refs[: 2 * count], refs[2 * count :]
    if degree == 1:
        walkers_ref, partial_ref, hartree_ref, out_ref, running_ref = refs
        columns = walkers_ref.shape[0]
        term = walkers_ref[...]
        running_ref[...] = term.astype(F32)
        points = 2 * count * field_ref.shape[2]
        row = energy_row(partial_ref.shape[0], occupied, columns, partial_ref, hartree_ref, points)
        out_ref[columns:, :128] = jnp.broadcast_to(row, (8, 128))
    else:
        own_ref, other_ref, before_ref, out_ref, running_ref = refs
        columns = before_ref.shape[0]
        term, running = step_term(degree - 1, own_ref, other_ref, before_ref)
        running_ref[...] = running
    first = where_ref[count]
    total = None
    for number in range(count):
        x = jnp.concatenate([blocks[2 * number][...], blocks[2 * number + 1][...]], axis=0)
        current = mm(term, x, NT).astype(BF16).astype(F32)
        field = field_ref[where_ref[number]]
        column = lax.broadcasted_iota(jnp.int32, current.shape, 0)
        scaled = jnp.where(column < first, field[0:1], field[1:2]) * current
        piece = mm(scaled.astype(BF16), x)
        total = piece if total is None else total + piece
    out_ref[:columns] = total


def degree_call(where, fields, blocks, degree, occupied, columns, *rest):
    count = len(blocks)
    rows, orbitals = fields.shape[2], blocks[0][0].shape[1]
    flat = [piece for block in blocks for piece in block]
    return pl.pallas_call(
        functools.partial(degree_kernel, count, degree, occupied),
        out_shape=(
            jax.ShapeDtypeStruct((columns + 8 if degree == 1 else columns, orbitals), F32),
            jax.ShapeDtypeStruct((columns, orbitals), F32),
        ),
        in_specs=[smem()] + [vmem()] * (1 + len(flat) + len(rest)),
        out_specs=(vmem(), vmem()),
        compiler_params=params(),
        cost_estimate=cost(4 * rows * count * orbitals * columns, 6e6),
        name="degree",
    )(where, fields, *flat, *rest)


def finish_kernel(where_ref, own_ref, other_ref, before_ref, own_energy, other_energy, out_ref, turned_ref):
    columns, orbitals = before_ref.shape
    chips, own_rows, lanes = out_ref.shape
    parity = where_ref[2]
    _, running = step_term(TAYLOR, own_ref, other_ref, before_ref)
    padded = jnp.concatenate([running, jnp.zeros((lanes - columns, orbitals), F32)], axis=0)
    turned_ref[...] = padded.T
    energy = own_energy[:, :lanes] + other_energy[:, :lanes]
    top = energy.astype(BF16).astype(F32)
    middle = (energy - top).astype(BF16).astype(F32)
    low = energy - top - middle
    row = lax.broadcasted_iota(jnp.int32, (own_rows, lanes), 0)
    lane = lax.broadcasted_iota(jnp.int32, (own_rows, lanes), 1)
    extra = jnp.where(row == 0, top[0:1], jnp.where(row == 1, middle[0:1], jnp.where(row == 2, low[0:1], 0.0)))
    for chip in range(chips):
        mine = turned_ref[pl.ds((2 * chip + parity) * own_rows, own_rows)]
        out_ref[chip] = jnp.where(lane < columns, mine, extra).astype(BF16)


def finish_call(where, own, other, running, own_energy, other_energy, devices):
    columns, orbitals = running.shape
    return pl.pallas_call(
        finish_kernel,
        out_shape=jax.ShapeDtypeStruct((devices // 2, orbitals // devices, 128), BF16),
        in_specs=[smem()] + [vmem()] * 5,
        out_specs=vmem(),
        scratch_shapes=[pltpu.VMEM((orbitals, 128), F32)],
        compiler_params=params(),
        cost_estimate=cost(1e6, 2e6),
        name="finish",
    )(where, own, other, running, own_energy, other_energy)


def body(points_map, trial, core, walkers, draws):
    rows, orbitals = points_map.shape
    walker_count, occupied = walkers.shape[1:]
    devices = lax.axis_size("pts")
    chips = devices // 2
    me = lax.axis_index("pts")
    chip, parity = me // 2, me % 2
    swapped = [(i, i ^ 1) for i in range(devices)]
    forward = [(i, (i + 2) % devices) for i in range(devices)]
    backward = [(i, (i - 2) % devices) for i in range(devices)]
    same_core = [[2 * z + c for z in range(chips)] for c in range(2)]
    columns = walker_count * occupied // chips
    cut = rows // 2 // 16 * 16

    def swap(value):
        return lax.ppermute(value, "pts", swapped)

    own = (points_map[:cut], points_map[cut:])
    right, left = own, own
    blocks, offsets = [own], [0]

    def advance(right, left):
        right = tuple(lax.ppermute(piece, "pts", forward) for piece in right)
        left = tuple(lax.ppermute(piece, "pts", backward) for piece in left)
        return right, left

    mate = swap(points_map)
    place = jnp.stack([me, me ^ 1, parity, chip]).astype(jnp.int32)
    turned = walkers.reshape(orbitals, walker_count * occupied).T
    trial_blocks = trial.reshape(devices, rows, occupied)
    orbit, near, sent = orbit_call(place, points_map, mate, turned, trial_blocks)
    mine = lax.all_to_all(
        sent, "pts", split_axis=0, concat_axis=0, tiled=True, axis_index_groups=same_core
    )
    theirs = swap(mine)
    cores = split_call(place, core, rows)
    came = swap(cores[1:2])
    outgoing, hartree = field_call(place, mine, theirs, cores, draws.T, occupied, columns)
    fields = lax.all_to_all(
        outgoing, "pts", split_axis=0, concat_axis=0, tiled=True, axis_index_groups=same_core
    )

    def exchange(offset, block, before, weight):
        far = (chip + offset) % chips
        where = jnp.stack([far, 2 * far + parity]).astype(jnp.int32)
        return exchange_call(
            where, block, turned, orbit, near, trial_blocks, cores, came, before, weight
        )

    def held(pieces, partial):
        out = []
        for piece in pieces:
            piece, partial = lax.optimization_barrier((piece, partial))
            out.append(piece)
        return tuple(out), partial

    partial = jnp.zeros((walker_count, 8, rows), F32)
    partial, fields = lax.optimization_barrier((partial, fields))
    half = chips // 2
    pending = (0, own, 1.0)
    for step in range(1, half):
        if step > 2:
            right, partial = held(right, partial)
            left, partial = held(left, partial)
        right, left = advance(right, left)
        partial = exchange(pending[0], pending[1], partial, pending[2])
        blocks += [right, left]
        offsets += [-step, step]
        pending = (-step, right, 2.0) if step % 2 else (step, left, 2.0)
    right, partial = held(right, partial)
    left, partial = held(left, partial)
    far_block = (lax.ppermute(right[0], "pts", forward), lax.ppermute(left[1], "pts", backward))
    partial = exchange(pending[0], pending[1], partial, pending[2])
    blocks.append(far_block)
    offsets.append(half)
    partial = exchange(half, far_block, partial, 1.0)

    start = chip * columns
    first_count = occupied - start % occupied
    sources = (chip + jnp.asarray(offsets, jnp.int32)) % chips
    where = jnp.concatenate([sources, first_count.reshape(1)]).astype(jnp.int32)
    term = lax.dynamic_slice_in_dim(turned, start, columns, 0)
    mine, running = degree_call(
        where, fields, blocks, 1, occupied, columns, term, partial, hartree
    )
    theirs = swap(mine)
    energies = (mine[columns:], theirs[columns:])
    for degree in range(2, TAYLOR + 1):
        mine, running = degree_call(
            where, fields, blocks, degree, occupied, columns, mine, theirs, running
        )
        theirs = swap(mine)
    message = finish_call(place, mine, theirs, running, *energies, devices)
    arrived = lax.all_to_all(
        message, "pts", split_axis=0, concat_axis=0, tiled=True, axis_index_groups=same_core
    )
    new_walkers = jnp.moveaxis(arrived[:, :, :columns], 0, 1)
    new_walkers = new_walkers.reshape(orbitals // devices, walker_count, occupied)
    energy = jnp.sum(arrived[:, :3, columns : columns + walker_count].astype(F32), axis=(0, 1))
    return (new_walkers, energy)


def solution(mesh):
    placed = (
        P(("mol", "pts"), None),
        P("mol", None),
        P(("mol", "pts"), None),
        P("mol", None, None),
        P(("mol", "pts"), None),
    )
    return jax.shard_map(
        body,
        mesh=mesh,
        in_specs=placed,
        out_specs=(P(("mol", "pts"), None, None), P("mol")),
        check_vma=False,
    )
```

```python
import functools
import math

import jax
import jax.numpy as jnp
from jax import lax
from jax.experimental import pallas as pl
from jax.experimental.pallas import tpu as pltpu
from jax.sharding import PartitionSpec as P

TAYLOR = 3
GAUSS_NODES = (-2.3344142, -0.7419637, 0.7419637, 2.3344142)
FIELD_STEP = 0.15
BF16, F32 = jnp.bfloat16, jnp.float32
NT = (((1,), (1,)), ((), ()))
NN = (((1,), (0,)), ((), ()))
VMEM_LIMIT = 24 * 1024 * 1024


def mm(a, b, dims=NN):
    return lax.dot_general(a, b, dims, preferred_element_type=F32)


def node_lookup(draws):
    values = jnp.zeros(draws.shape, F32)
    for number, node in enumerate(GAUSS_NODES):
        values = values + jnp.where(draws == number, node, 0.0).astype(F32)
    return values


def vmem():
    return pl.BlockSpec(memory_space=pltpu.VMEM)


def cost(flops, moved):
    return pl.CostEstimate(flops=int(flops), bytes_accessed=int(moved), transcendentals=0)


def params():
    return pltpu.CompilerParams(vmem_limit_bytes=VMEM_LIMIT)


def anywhere():
    return pl.BlockSpec(memory_space=pl.ANY)


def position():
    me = lax.axis_index("pts")
    chip = lax.div(me, 2)
    return me, chip, me - 2 * chip


def orbit_kernel(occupied, own_ref, mate_ref, w_ref, trial_any, orbit_ref, near_ref, sent_ref, trial_ref, sems):
    me, _, parity = position()
    copies = [
        pltpu.make_async_copy(trial_any.at[device], trial_ref.at[k], sems.at[k])
        for k, device in enumerate((me, me + 1 - 2 * parity))
    ]
    for copy in copies:
        copy.start()
    rows = own_ref.shape[0]
    x = jnp.concatenate([own_ref[...].astype(F32), mate_ref[...].astype(F32)], axis=0).astype(BF16)
    for copy in copies:
        copy.wait()
    trial = trial_ref[0].astype(F32)
    near = jnp.concatenate([trial, trial_ref[1].astype(F32)], axis=0)
    near_ref[...] = near.astype(BF16)
    lane = lax.broadcasted_iota(jnp.int32, (rows, 128), 1)
    density = jnp.zeros((rows, 128), F32)
    for pair in range(w_ref.shape[0] // (2 * occupied)):
        both = mm(x, w_ref[pair * 2 * occupied : (pair + 1) * 2 * occupied], NT).astype(BF16)
        for half in range(2):
            one = both[:, half * occupied : (half + 1) * occupied]
            walker = 2 * pair + half
            orbit_ref[walker] = one
            total = jnp.sum(one.astype(F32)[:rows] * trial, axis=1, keepdims=True)
            density = jnp.where(lane == walker, total / math.sqrt(occupied), density)
    turned = density.T[: sent_ref.shape[1]].astype(BF16)
    for device in range(sent_ref.shape[0]):
        sent_ref[device] = turned


def orbit_call(own, mate, turned_walkers, trial_blocks):
    rows, orbitals = own.shape
    devices, _, occupied = trial_blocks.shape
    walkers = turned_walkers.shape[0] // occupied
    return pl.pallas_call(
        functools.partial(orbit_kernel, occupied),
        out_shape=(
            jax.ShapeDtypeStruct((walkers, 2 * rows, occupied), BF16),
            jax.ShapeDtypeStruct((2 * rows, occupied), BF16),
            jax.ShapeDtypeStruct((devices // 2, -(-walkers // 16) * 16, rows), BF16),
        ),
        in_specs=[vmem()] * 3 + [anywhere()],
        out_specs=(vmem(), vmem(), vmem()),
        scratch_shapes=[pltpu.VMEM((2, rows, occupied), BF16), pltpu.SemaphoreType.DMA((2,))],
        compiler_params=params(),
        cost_estimate=cost(4 * rows * orbitals * walkers * occupied, 6e6),
        name="orbit",
    )(own, mate, turned_walkers, trial_blocks)


def split_kernel(core_ref, out_ref):
    width = out_ref.shape[3]
    _, _, parity = position()
    for block in range(core_ref.shape[1] // width):
        slot = lax.rem(block % 2 + parity, 2)
        out_ref[slot, block // 2] = core_ref[:, block * width : (block + 1) * width]


def split_call(core, width):
    rows, columns = core.shape
    return pl.pallas_call(
        split_kernel,
        out_shape=jax.ShapeDtypeStruct((2, columns // width // 2, rows, width), BF16),
        in_specs=[vmem()],
        out_specs=vmem(),
        compiler_params=params(),
        cost_estimate=cost(1e6, 6e6),
        name="split",
    )(core)


def field_kernel(walkers, occupied, columns, mine_ref, theirs_ref, cores_ref, draws_ref, out_ref, hartree_ref):
    total = None
    for chip in range(cores_ref.shape[1]):
        for slot, density_ref in enumerate((mine_ref, theirs_ref)):
            piece = mm(density_ref[chip], cores_ref[slot, chip], NT)
            total = piece if total is None else total + piece
    mine = mine_ref[position()[1]].astype(F32)
    hartree_ref[...] = jnp.broadcast_to(jnp.sum(mine * total, axis=1, keepdims=True), hartree_ref.shape)
    field = FIELD_STEP * (node_lookup(draws_ref[...]) - FIELD_STEP * total[:walkers])
    for chip in range(out_ref.shape[0]):
        first = columns * chip // occupied
        out_ref[chip, 0:1] = field[first : first + 1]
        second = min(first + 1, walkers - 1)
        out_ref[chip, 1:2] = field[second : second + 1]


def field_call(mine, theirs, cores, draws, occupied, columns):
    chips, padded, rows = mine.shape
    walkers = draws.shape[0]
    return pl.pallas_call(
        functools.partial(field_kernel, walkers, occupied, columns),
        out_shape=(
            jax.ShapeDtypeStruct((chips, 2, rows), F32),
            jax.ShapeDtypeStruct((padded, 128), F32),
        ),
        in_specs=[vmem()] * 4,
        out_specs=(vmem(), vmem()),
        compiler_params=params(),
        cost_estimate=cost(4e9, 4e6),
        name="field",
    )(mine, theirs, cores, draws)


def exchange_kernel(
    occupied, weight, offset, upper_ref, lower_ref, w_ref, orbit_ref, near_ref, before_ref, trial_any, cores_any,
    came_any, out_ref, core_ref, far_ref, forward_ref, backward_ref, trial_ref, half_ref, sems,
):
    _, chip, parity = position()
    chips = cores_any.shape[1]
    far = lax.rem(chip + (offset + chips), chips)
    copies = [
        pltpu.make_async_copy(trial_any.at[2 * far + parity], trial_ref, sems.at[0]),
        pltpu.make_async_copy(cores_any.at[0, far], half_ref.at[0], sems.at[1]),
        pltpu.make_async_copy(came_any.at[0, far], half_ref.at[1], sems.at[2]),
    ]
    for copy in copies:
        copy.start()
    x = jnp.concatenate([upper_ref[...], lower_ref[...]], axis=0)
    rows = x.shape[0]
    far_ref[...] = mm(w_ref[...], x, NT).astype(BF16)
    for copy in copies:
        copy.wait()
    core_ref[:rows] = half_ref[0].astype(F32)
    core_ref[rows:] = half_ref[1].astype(F32)
    far_trial = trial_ref[...]
    walkers = out_ref.shape[0]
    forward_ref[1] = jnp.zeros(core_ref.shape, F32)
    backward_ref[1] = jnp.zeros(core_ref.shape, F32)

    def gather(walker, slot):
        value = forward_ref[slot] * backward_ref[slot] * core_ref[...]
        total = jnp.sum(value.reshape(-1, 8, rows), axis=0)
        out_ref[walker] = before_ref[walker] + weight * total

    def spread(walker, slot):
        orbit_far = far_ref[pl.ds(pl.multiple_of(walker * occupied, occupied), occupied)]
        forward_ref[slot] = mm(orbit_ref[walker], far_trial, NT)
        backward_ref[slot] = mm(near_ref[...], orbit_far)

    def two(number, carry):
        gather(lax.rem(2 * number + walkers - 1, walkers), 1)
        spread(2 * number, 0)
        gather(2 * number, 0)
        spread(2 * number + 1, 1)
        return carry

    lax.fori_loop(0, walkers // 2, two, 0)
    gather(walkers - 1, 1)


def exchange_call(offset, block, turned_walkers, orbit, near, trial_blocks, cores, came, before, weight):
    walkers, near_rows, occupied = orbit.shape
    rows = came.shape[2]
    orbitals = turned_walkers.shape[1]
    return pl.pallas_call(
        functools.partial(exchange_kernel, occupied, weight, offset),
        out_shape=jax.ShapeDtypeStruct(before.shape, F32),
        in_specs=[vmem()] * 6 + [anywhere()] * 3,
        out_specs=vmem(),
        scratch_shapes=[
            pltpu.VMEM((near_rows, rows), F32),
            pltpu.VMEM((walkers * occupied, rows), BF16),
            pltpu.VMEM((2, near_rows, rows), F32),
            pltpu.VMEM((2, near_rows, rows), F32),
            pltpu.VMEM((rows, occupied), BF16),
            pltpu.VMEM((2, rows, rows), BF16),
            pltpu.SemaphoreType.DMA((3,)),
        ],
        compiler_params=params(),
        cost_estimate=cost(2 * rows * walkers * occupied * (orbitals + 4 * rows), 5e6),
        name="exchange",
    )(*block, turned_walkers, orbit, near, before, trial_blocks, cores, came)


def energy_row(walkers, occupied, shift, partial_ref, hartree_ref, points):
    exchange = jnp.sum(jnp.sum(partial_ref[...], axis=1), axis=1, keepdims=True) / occupied
    energy = (hartree_ref[:walkers] - exchange) / (2.0 * points)
    row = lax.broadcasted_iota(jnp.int32, energy.shape, 0)
    lane = lax.broadcasted_iota(jnp.int32, energy.shape, 1)
    return jnp.sum(jnp.where(lane == row + shift, energy, 0.0), axis=0, keepdims=True)


def step_term(degree, own_ref, other_ref, running_ref):
    columns = running_ref.shape[0]
    term = ((own_ref[:columns] + other_ref[:columns]) / degree).astype(BF16)
    return term, running_ref[...] + term.astype(F32)


def degree_kernel(offsets, degree, occupied, field_ref, *refs):
    count = len(offsets)
    _, chip, _ = position()
    blocks, refs = refs[: 2 * count], refs[2 * count :]
    if degree == 1:
        walkers_any, partial_ref, hartree_ref, out_ref, running_ref, walkers_ref, sem = refs
        columns = walkers_ref.shape[0]
        start = pl.multiple_of(chip * columns, math.gcd(columns, 32))
        copy = pltpu.make_async_copy(walkers_any.at[pl.ds(start, columns)], walkers_ref, sem)
        copy.start()
        copy.wait()
        term = walkers_ref[...]
        running_ref[...] = term.astype(F32)
        points = 2 * count * field_ref.shape[2]
        row = energy_row(partial_ref.shape[0], occupied, columns, partial_ref, hartree_ref, points)
        out_ref[columns:, :128] = jnp.broadcast_to(row, (8, 128))
    else:
        own_ref, other_ref, before_ref, out_ref, running_ref = refs
        columns = before_ref.shape[0]
        term, running = step_term(degree - 1, own_ref, other_ref, before_ref)
        running_ref[...] = running
    first = occupied - lax.rem(chip * columns, occupied)
    total = None
    for number in range(count):
        x = jnp.concatenate([blocks[2 * number][...], blocks[2 * number + 1][...]], axis=0)
        current = mm(term, x, NT).astype(BF16).astype(F32)
        field = field_ref[lax.rem(chip + (offsets[number] + count), count)]
        column = lax.broadcasted_iota(jnp.int32, current.shape, 0)
        scaled = jnp.where(column < first, field[0:1], field[1:2]) * current
        piece = mm(scaled.astype(BF16), x)
        total = piece if total is None else total + piece
    out_ref[:columns] = total


def degree_call(offsets, fields, blocks, degree, occupied, columns, *rest):
    count = len(blocks)
    rows, orbitals = fields.shape[2], blocks[0][0].shape[1]
    flat = [piece for block in blocks for piece in block]
    return pl.pallas_call(
        functools.partial(degree_kernel, tuple(offsets), degree, occupied),
        out_shape=(
            jax.ShapeDtypeStruct((columns + 8 if degree == 1 else columns, orbitals), F32),
            jax.ShapeDtypeStruct((columns, orbitals), F32),
        ),
        in_specs=[vmem()] * (1 + len(flat))
        + [anywhere() if degree == 1 else vmem()]
        + [vmem()] * (len(rest) - 1),
        out_specs=(vmem(), vmem()),
        scratch_shapes=[pltpu.VMEM((columns, orbitals), BF16), pltpu.SemaphoreType.DMA(())]
        if degree == 1
        else [],
        compiler_params=params(),
        cost_estimate=cost(4 * rows * count * orbitals * columns, 6e6),
        name="degree",
    )(fields, *flat, *rest)


def finish_kernel(own_ref, other_ref, before_ref, own_energy, other_energy, out_ref, turned_ref):
    columns, orbitals = before_ref.shape
    chips, own_rows, lanes = out_ref.shape
    _, _, parity = position()
    _, running = step_term(TAYLOR, own_ref, other_ref, before_ref)
    padded = jnp.concatenate([running, jnp.zeros((lanes - columns, orbitals), F32)], axis=0)
    turned_ref[...] = padded.T
    energy = own_energy[:, :lanes] + other_energy[:, :lanes]
    top = energy.astype(BF16).astype(F32)
    middle = (energy - top).astype(BF16).astype(F32)
    low = energy - top - middle
    row = lax.broadcasted_iota(jnp.int32, (own_rows, lanes), 0)
    lane = lax.broadcasted_iota(jnp.int32, (own_rows, lanes), 1)
    extra = jnp.where(row == 0, top[0:1], jnp.where(row == 1, middle[0:1], jnp.where(row == 2, low[0:1], 0.0)))
    for chip in range(chips):
        mine = turned_ref[pl.ds((2 * chip + parity) * own_rows, own_rows)]
        out_ref[chip] = jnp.where(lane < columns, mine, extra).astype(BF16)


def finish_call(own, other, running, own_energy, other_energy, devices):
    columns, orbitals = running.shape
    return pl.pallas_call(
        finish_kernel,
        out_shape=jax.ShapeDtypeStruct((devices // 2, orbitals // devices, 128), BF16),
        in_specs=[vmem()] * 5,
        out_specs=vmem(),
        scratch_shapes=[pltpu.VMEM((orbitals, 128), F32)],
        compiler_params=params(),
        cost_estimate=cost(1e6, 2e6),
        name="finish",
    )(own, other, running, own_energy, other_energy)


def body(points_map, trial, core, walkers, draws):
    rows, orbitals = points_map.shape
    walker_count, occupied = walkers.shape[1:]
    devices = lax.axis_size("pts")
    chips = devices // 2
    swapped = [(i, i ^ 1) for i in range(devices)]
    forward = [(i, (i + 2) % devices) for i in range(devices)]
    backward = [(i, (i - 2) % devices) for i in range(devices)]
    same_core = [[2 * z + c for z in range(chips)] for c in range(2)]
    columns = walker_count * occupied // chips
    cut = rows // 2 // 16 * 16

    def swap(value):
        return lax.ppermute(value, "pts", swapped)

    own = (points_map[:cut], points_map[cut:])
    right, left = own, own
    blocks, offsets = [own], [0]

    def advance(right, left):
        right = tuple(lax.ppermute(piece, "pts", forward) for piece in right)
        left = tuple(lax.ppermute(piece, "pts", backward) for piece in left)
        return right, left

    mate = swap(points_map)
    turned = walkers.reshape(orbitals, walker_count * occupied).T
    trial_blocks = trial.reshape(devices, rows, occupied)
    orbit, near, sent = orbit_call(points_map, mate, turned, trial_blocks)
    mine = lax.all_to_all(
        sent, "pts", split_axis=0, concat_axis=0, tiled=True, axis_index_groups=same_core
    )
    theirs = swap(mine)
    cores = split_call(core, rows)
    came = swap(cores[1:2])
    outgoing, hartree = field_call(mine, theirs, cores, draws.T, occupied, columns)
    fields = lax.all_to_all(
        outgoing, "pts", split_axis=0, concat_axis=0, tiled=True, axis_index_groups=same_core
    )

    def exchange(offset, block, before, weight):
        return exchange_call(
            offset, block, turned, orbit, near, trial_blocks, cores, came, before, weight
        )

    def held(pieces, partial):
        out = []
        for piece in pieces:
            piece, partial = lax.optimization_barrier((piece, partial))
            out.append(piece)
        return tuple(out), partial

    partial = jnp.zeros((walker_count, 8, rows), F32)
    partial, fields = lax.optimization_barrier((partial, fields))
    half = chips // 2
    pending = (0, own, 1.0)
    for step in range(1, half):
        if step > 2:
            right, partial = held(right, partial)
            left, partial = held(left, partial)
        right, left = advance(right, left)
        partial = exchange(pending[0], pending[1], partial, pending[2])
        blocks += [right, left]
        offsets += [-step, step]
        pending = (-step, right, 2.0) if step % 2 else (step, left, 2.0)
    right, partial = held(right, partial)
    left, partial = held(left, partial)
    far_block = (lax.ppermute(right[0], "pts", forward), lax.ppermute(left[1], "pts", backward))
    partial = exchange(pending[0], pending[1], partial, pending[2])
    blocks.append(far_block)
    offsets.append(half)
    partial = exchange(half, far_block, partial, 1.0)

    mine, running = degree_call(
        offsets, fields, blocks, 1, occupied, columns, turned, partial, hartree
    )
    theirs = swap(mine)
    energies = (mine[columns:], theirs[columns:])
    for degree in range(2, TAYLOR + 1):
        mine, running = degree_call(
            offsets, fields, blocks, degree, occupied, columns, mine, theirs, running
        )
        theirs = swap(mine)
    message = finish_call(mine, theirs, running, *energies, devices)
    arrived = lax.all_to_all(
        message, "pts", split_axis=0, concat_axis=0, tiled=True, axis_index_groups=same_core
    )
    new_walkers = jnp.moveaxis(arrived[:, :, :columns], 0, 1)
    new_walkers = new_walkers.reshape(orbitals // devices, walker_count, occupied)
    energy = jnp.sum(arrived[:, :3, columns : columns + walker_count].astype(F32), axis=(0, 1))
    return (new_walkers, energy)


def solution(mesh):
    placed = (
        P(("mol", "pts"), None),
        P("mol", None),
        P(("mol", "pts"), None),
        P("mol", None, None),
        P(("mol", "pts"), None),
    )
    return jax.shard_map(
        body,
        mesh=mesh,
        in_specs=placed,
        out_specs=(P(("mol", "pts"), None, None), P("mol")),
        check_vma=False,
    )
```

```python
import functools
import math

import jax
import jax.numpy as jnp
from jax import lax
from jax.experimental import pallas as pl
from jax.experimental.pallas import tpu as pltpu
from jax.sharding import PartitionSpec as P

TAYLOR = 3
GAUSS_NODES = (-2.3344142, -0.7419637, 0.7419637, 2.3344142)
FIELD_STEP = 0.15
BF16, F32 = jnp.bfloat16, jnp.float32
NT = (((1,), (1,)), ((), ()))
NN = (((1,), (0,)), ((), ()))
VMEM_LIMIT = 24 * 1024 * 1024


def mm(a, b, dims=NN):
    return lax.dot_general(a, b, dims, preferred_element_type=F32)


def node_lookup(draws):
    values = jnp.zeros(draws.shape, F32)
    for number, node in enumerate(GAUSS_NODES):
        values = values + jnp.where(draws == number, node, 0.0).astype(F32)
    return values


def vmem():
    return pl.BlockSpec(memory_space=pltpu.VMEM)


def cost(flops, moved):
    return pl.CostEstimate(flops=int(flops), bytes_accessed=int(moved), transcendentals=0)


def params():
    return pltpu.CompilerParams(vmem_limit_bytes=VMEM_LIMIT)


def anywhere():
    return pl.BlockSpec(memory_space=pl.ANY)


def position():
    me = lax.axis_index("pts")
    chip = lax.div(me, 2)
    return me, chip, me - 2 * chip


def orbit_kernel(occupied, own_ref, mate_ref, w_ref, trial_any, orbit_ref, near_ref, sent_ref, trial_ref, sems):
    me, _, parity = position()
    copies = [
        pltpu.make_async_copy(trial_any.at[device], trial_ref.at[k], sems.at[k])
        for k, device in enumerate((me, me + 1 - 2 * parity))
    ]
    for copy in copies:
        copy.start()
    rows = own_ref.shape[0]
    x = jnp.concatenate([own_ref[...].astype(F32), mate_ref[...].astype(F32)], axis=0).astype(BF16)
    for copy in copies:
        copy.wait()
    trial = trial_ref[0].astype(F32)
    near = jnp.concatenate([trial, trial_ref[1].astype(F32)], axis=0)
    near_ref[...] = near.astype(BF16)
    lane = lax.broadcasted_iota(jnp.int32, (rows, 128), 1)
    density = jnp.zeros((rows, 128), F32)
    for pair in range(w_ref.shape[0] // (2 * occupied)):
        both = mm(x, w_ref[pair * 2 * occupied : (pair + 1) * 2 * occupied], NT).astype(BF16)
        for half in range(2):
            one = both[:, half * occupied : (half + 1) * occupied]
            walker = 2 * pair + half
            orbit_ref[walker] = one
            total = jnp.sum(one.astype(F32)[:rows] * trial, axis=1, keepdims=True)
            density = jnp.where(lane == walker, total / math.sqrt(occupied), density)
    turned = density.T[: sent_ref.shape[1]].astype(BF16)
    for device in range(sent_ref.shape[0]):
        sent_ref[device] = turned


def orbit_call(own, mate, turned_walkers, trial_blocks):
    rows, orbitals = own.shape
    devices, _, occupied = trial_blocks.shape
    walkers = turned_walkers.shape[0] // occupied
    return pl.pallas_call(
        functools.partial(orbit_kernel, occupied),
        out_shape=(
            jax.ShapeDtypeStruct((walkers, 2 * rows, occupied), BF16),
            jax.ShapeDtypeStruct((2 * rows, occupied), BF16),
            jax.ShapeDtypeStruct((devices // 2, -(-walkers // 16) * 16, rows), BF16),
        ),
        in_specs=[vmem()] * 3 + [anywhere()],
        out_specs=(vmem(), vmem(), vmem()),
        scratch_shapes=[pltpu.VMEM((2, rows, occupied), BF16), pltpu.SemaphoreType.DMA((2,))],
        compiler_params=params(),
        cost_estimate=cost(4 * rows * orbitals * walkers * occupied, 6e6),
        name="orbit",
    )(own, mate, turned_walkers, trial_blocks)


def split_kernel(core_ref, out_ref):
    width = out_ref.shape[3]
    _, _, parity = position()
    for block in range(core_ref.shape[1] // width):
        slot = lax.rem(block % 2 + parity, 2)
        out_ref[slot, block // 2] = core_ref[:, block * width : (block + 1) * width]


def split_call(core, width):
    rows, columns = core.shape
    return pl.pallas_call(
        split_kernel,
        out_shape=jax.ShapeDtypeStruct((2, columns // width // 2, rows, width), BF16),
        in_specs=[vmem()],
        out_specs=vmem(),
        compiler_params=params(),
        cost_estimate=cost(1e6, 6e6),
        name="split",
    )(core)


def field_kernel(walkers, occupied, columns, mine_ref, theirs_ref, cores_ref, draws_ref, out_ref, hartree_ref):
    total = None
    for chip in range(cores_ref.shape[1]):
        for slot, density_ref in enumerate((mine_ref, theirs_ref)):
            piece = mm(density_ref[chip], cores_ref[slot, chip], NT)
            total = piece if total is None else total + piece
    mine = mine_ref[position()[1]].astype(F32)
    hartree_ref[...] = jnp.broadcast_to(jnp.sum(mine * total, axis=1, keepdims=True), hartree_ref.shape)
    field = FIELD_STEP * (node_lookup(draws_ref[...]) - FIELD_STEP * total[:walkers])
    for chip in range(out_ref.shape[0]):
        first = columns * chip // occupied
        out_ref[chip, 0:1] = field[first : first + 1]
        second = min(first + 1, walkers - 1)
        out_ref[chip, 1:2] = field[second : second + 1]


def field_call(mine, theirs, cores, draws, occupied, columns):
    chips, padded, rows = mine.shape
    walkers = draws.shape[0]
    return pl.pallas_call(
        functools.partial(field_kernel, walkers, occupied, columns),
        out_shape=(
            jax.ShapeDtypeStruct((chips, 2, rows), F32),
            jax.ShapeDtypeStruct((padded, 128), F32),
        ),
        in_specs=[vmem()] * 4,
        out_specs=(vmem(), vmem()),
        compiler_params=params(),
        cost_estimate=cost(4e9, 4e6),
        name="field",
    )(mine, theirs, cores, draws)


def exchange_kernel(
    occupied, weight, offset, x_ref, w_ref, orbit_ref, near_ref, before_ref, trial_any, cores_any,
    came_any, out_ref, core_ref, far_ref, forward_ref, backward_ref, trial_ref, half_ref, sems,
):
    _, chip, parity = position()
    chips = cores_any.shape[1]
    far = lax.rem(chip + (offset + chips), chips)
    copies = [
        pltpu.make_async_copy(trial_any.at[2 * far + parity], trial_ref, sems.at[0]),
        pltpu.make_async_copy(cores_any.at[0, far], half_ref.at[0], sems.at[1]),
        pltpu.make_async_copy(came_any.at[0, far], half_ref.at[1], sems.at[2]),
    ]
    for copy in copies:
        copy.start()
    x = x_ref[...]
    rows = x.shape[0]
    far_ref[...] = mm(w_ref[...], x, NT).astype(BF16)
    for copy in copies:
        copy.wait()
    core_ref[:rows] = half_ref[0].astype(F32)
    core_ref[rows:] = half_ref[1].astype(F32)
    far_trial = trial_ref[...]
    walkers = out_ref.shape[0]
    forward_ref[1] = jnp.zeros(core_ref.shape, F32)
    backward_ref[1] = jnp.zeros(core_ref.shape, F32)

    def gather(walker, slot):
        value = forward_ref[slot] * backward_ref[slot] * core_ref[...]
        total = jnp.sum(value.reshape(-1, 8, rows), axis=0)
        out_ref[walker] = before_ref[walker] + weight * total

    def spread(walker, slot):
        orbit_far = far_ref[pl.ds(pl.multiple_of(walker * occupied, occupied), occupied)]
        forward_ref[slot] = mm(orbit_ref[walker], far_trial, NT)
        backward_ref[slot] = mm(near_ref[...], orbit_far)

    def two(number, carry):
        gather(lax.rem(2 * number + walkers - 1, walkers), 1)
        spread(2 * number, 0)
        gather(2 * number, 0)
        spread(2 * number + 1, 1)
        return carry

    lax.fori_loop(0, walkers // 2, two, 0)
    gather(walkers - 1, 1)


def exchange_call(offset, block, turned_walkers, orbit, near, trial_blocks, cores, came, before, weight):
    walkers, near_rows, occupied = orbit.shape
    rows = came.shape[2]
    orbitals = turned_walkers.shape[1]
    return pl.pallas_call(
        functools.partial(exchange_kernel, occupied, weight, offset),
        out_shape=jax.ShapeDtypeStruct(before.shape, F32),
        in_specs=[vmem()] * 5 + [anywhere()] * 3,
        out_specs=vmem(),
        scratch_shapes=[
            pltpu.VMEM((near_rows, rows), F32),
            pltpu.VMEM((walkers * occupied, rows), BF16),
            pltpu.VMEM((2, near_rows, rows), F32),
            pltpu.VMEM((2, near_rows, rows), F32),
            pltpu.VMEM((rows, occupied), BF16),
            pltpu.VMEM((2, rows, rows), BF16),
            pltpu.SemaphoreType.DMA((3,)),
        ],
        compiler_params=params(),
        cost_estimate=cost(2 * rows * walkers * occupied * (orbitals + 4 * rows), 5e6),
        name="exchange",
    )(block, turned_walkers, orbit, near, before, trial_blocks, cores, came)


def energy_row(walkers, occupied, shift, partial_ref, hartree_ref, points):
    exchange = jnp.sum(jnp.sum(partial_ref[...], axis=1), axis=1, keepdims=True) / occupied
    energy = (hartree_ref[:walkers] - exchange) / (2.0 * points)
    row = lax.broadcasted_iota(jnp.int32, energy.shape, 0)
    lane = lax.broadcasted_iota(jnp.int32, energy.shape, 1)
    return jnp.sum(jnp.where(lane == row + shift, energy, 0.0), axis=0, keepdims=True)


def step_term(degree, own_ref, other_ref, running_ref):
    columns = running_ref.shape[0]
    term = ((own_ref[:columns] + other_ref[:columns]) / degree).astype(BF16)
    return term, running_ref[...] + term.astype(F32)


def degree_kernel(offsets, degree, occupied, field_ref, *refs):
    count = len(offsets)
    _, chip, _ = position()
    blocks, refs = refs[:count], refs[count:]
    if degree == 1:
        walkers_any, partial_ref, hartree_ref, out_ref, running_ref, walkers_ref, sem = refs
        columns = walkers_ref.shape[0]
        start = pl.multiple_of(chip * columns, math.gcd(columns, 32))
        copy = pltpu.make_async_copy(walkers_any.at[pl.ds(start, columns)], walkers_ref, sem)
        copy.start()
        copy.wait()
        term = walkers_ref[...]
        running_ref[...] = term.astype(F32)
        points = 2 * count * field_ref.shape[2]
        row = energy_row(partial_ref.shape[0], occupied, columns, partial_ref, hartree_ref, points)
        out_ref[columns:, :128] = jnp.broadcast_to(row, (8, 128))
    else:
        own_ref, other_ref, before_ref, out_ref, running_ref = refs
        columns = before_ref.shape[0]
        term, running = step_term(degree - 1, own_ref, other_ref, before_ref)
        running_ref[...] = running
    first = occupied - lax.rem(chip * columns, occupied)
    total = None
    for number in range(count):
        x = blocks[number][...]
        current = mm(term, x, NT).astype(BF16).astype(F32)
        field = field_ref[lax.rem(chip + (offsets[number] + count), count)]
        column = lax.broadcasted_iota(jnp.int32, current.shape, 0)
        scaled = jnp.where(column < first, field[0:1], field[1:2]) * current
        piece = mm(scaled.astype(BF16), x)
        total = piece if total is None else total + piece
    out_ref[:columns] = total


def degree_call(offsets, fields, blocks, degree, occupied, columns, *rest):
    count = len(blocks)
    rows, orbitals = fields.shape[2], blocks[0].shape[1]
    return pl.pallas_call(
        functools.partial(degree_kernel, tuple(offsets), degree, occupied),
        out_shape=(
            jax.ShapeDtypeStruct((columns + 8 if degree == 1 else columns, orbitals), F32),
            jax.ShapeDtypeStruct((columns, orbitals), F32),
        ),
        in_specs=[vmem()] * (1 + count)
        + [anywhere() if degree == 1 else vmem()]
        + [vmem()] * (len(rest) - 1),
        out_specs=(vmem(), vmem()),
        scratch_shapes=[pltpu.VMEM((columns, orbitals), BF16), pltpu.SemaphoreType.DMA(())]
        if degree == 1
        else [],
        compiler_params=params(),
        cost_estimate=cost(4 * rows * count * orbitals * columns, 6e6),
        name="degree",
    )(fields, *blocks, *rest)


def finish_kernel(own_ref, other_ref, before_ref, own_energy, other_energy, out_ref, turned_ref):
    columns, orbitals = before_ref.shape
    chips, own_rows, lanes = out_ref.shape
    _, _, parity = position()
    _, running = step_term(TAYLOR, own_ref, other_ref, before_ref)
    padded = jnp.concatenate([running, jnp.zeros((lanes - columns, orbitals), F32)], axis=0)
    turned_ref[...] = padded.T
    energy = own_energy[:, :lanes] + other_energy[:, :lanes]
    top = energy.astype(BF16).astype(F32)
    middle = (energy - top).astype(BF16).astype(F32)
    low = energy - top - middle
    row = lax.broadcasted_iota(jnp.int32, (own_rows, lanes), 0)
    lane = lax.broadcasted_iota(jnp.int32, (own_rows, lanes), 1)
    extra = jnp.where(row == 0, top[0:1], jnp.where(row == 1, middle[0:1], jnp.where(row == 2, low[0:1], 0.0)))
    for chip in range(chips):
        mine = turned_ref[pl.ds((2 * chip + parity) * own_rows, own_rows)]
        out_ref[chip] = jnp.where(lane < columns, mine, extra).astype(BF16)


def finish_call(own, other, running, own_energy, other_energy, devices):
    columns, orbitals = running.shape
    return pl.pallas_call(
        finish_kernel,
        out_shape=jax.ShapeDtypeStruct((devices // 2, orbitals // devices, 128), BF16),
        in_specs=[vmem()] * 5,
        out_specs=vmem(),
        scratch_shapes=[pltpu.VMEM((orbitals, 128), F32)],
        compiler_params=params(),
        cost_estimate=cost(1e6, 2e6),
        name="finish",
    )(own, other, running, own_energy, other_energy)


def body(points_map, trial, core, walkers, draws):
    rows, orbitals = points_map.shape
    walker_count, occupied = walkers.shape[1:]
    devices = lax.axis_size("pts")
    chips = devices // 2
    swapped = [(i, i ^ 1) for i in range(devices)]
    forward = [(i, (i + 2) % devices) for i in range(devices)]
    backward = [(i, (i - 2) % devices) for i in range(devices)]
    same_core = [[2 * z + c for z in range(chips)] for c in range(2)]
    columns = walker_count * occupied // chips

    def swap(value):
        return lax.ppermute(value, "pts", swapped)

    mate = swap(points_map)
    turned = walkers.reshape(orbitals, walker_count * occupied).T
    trial_blocks = trial.reshape(devices, rows, occupied)
    orbit, near, sent = orbit_call(points_map, mate, turned, trial_blocks)
    mine = lax.all_to_all(
        sent, "pts", split_axis=0, concat_axis=0, tiled=True, axis_index_groups=same_core
    )
    theirs = swap(mine)
    cores = split_call(core, rows)
    came = swap(cores[1:2])
    outgoing, hartree = field_call(mine, theirs, cores, draws.T, occupied, columns)
    fields = lax.all_to_all(
        outgoing, "pts", split_axis=0, concat_axis=0, tiled=True, axis_index_groups=same_core
    )

    def exchange(offset, block, before, weight):
        return exchange_call(
            offset, block, turned, orbit, near, trial_blocks, cores, came, before, weight
        )

    partial = jnp.zeros((walker_count, 8, rows), F32)
    partial, fields = lax.optimization_barrier((partial, fields))
    half = chips // 2
    right = left = points_map
    blocks, offsets = [points_map], [0]
    for step in range(half):
        if step > 1:
            right, partial = lax.optimization_barrier((right, partial))
        after = lax.ppermute(right, "pts", forward)
        partial = exchange(-step, right, partial, 2.0 if step else 1.0)
        if step > 1:
            left, partial = lax.optimization_barrier((left, partial))
        if step < half - 1:
            left = lax.ppermute(left, "pts", backward)
            blocks.append(left)
            offsets.append(step + 1)
        right = after
        blocks.append(right)
        offsets.append(-step - 1)
    partial = exchange(-half, right, partial, 1.0)

    mine, running = degree_call(
        offsets, fields, blocks, 1, occupied, columns, turned, partial, hartree
    )
    theirs = swap(mine)
    energies = (mine[columns:], theirs[columns:])
    for degree in range(2, TAYLOR + 1):
        mine, running = degree_call(
            offsets, fields, blocks, degree, occupied, columns, mine, theirs, running
        )
        theirs = swap(mine)
    message = finish_call(mine, theirs, running, *energies, devices)
    arrived = lax.all_to_all(
        message, "pts", split_axis=0, concat_axis=0, tiled=True, axis_index_groups=same_core
    )
    new_walkers = jnp.moveaxis(arrived[:, :, :columns], 0, 1)
    new_walkers = new_walkers.reshape(orbitals // devices, walker_count, occupied)
    energy = jnp.sum(arrived[:, :3, columns : columns + walker_count].astype(F32), axis=(0, 1))
    return (new_walkers, energy)


def solution(mesh):
    placed = (
        P(("mol", "pts"), None),
        P("mol", None),
        P(("mol", "pts"), None),
        P("mol", None, None),
        P(("mol", "pts"), None),
    )
    return jax.shard_map(
        body,
        mesh=mesh,
        in_specs=placed,
        out_specs=(P(("mol", "pts"), None, None), P("mol")),
        check_vma=False,
    )
```

```python
import functools
import math

import jax
import jax.numpy as jnp
from jax import lax
from jax.experimental import pallas as pl
from jax.experimental.pallas import tpu as pltpu
from jax.sharding import PartitionSpec as P

TAYLOR = 3
GAUSS_NODES = (-2.3344142, -0.7419637, 0.7419637, 2.3344142)
FIELD_STEP = 0.15
BF16, F32 = jnp.bfloat16, jnp.float32
NT = (((1,), (1,)), ((), ()))
NN = (((1,), (0,)), ((), ()))
VMEM_LIMIT = 24 * 1024 * 1024


def mm(a, b, dims=NN):
    return lax.dot_general(a, b, dims, preferred_element_type=F32)


def node_lookup(draws):
    values = jnp.zeros(draws.shape, F32)
    for number, node in enumerate(GAUSS_NODES):
        values = values + jnp.where(draws == number, node, 0.0).astype(F32)
    return values


def vmem():
    return pl.BlockSpec(memory_space=pltpu.VMEM)


def cost(flops, moved):
    return pl.CostEstimate(flops=int(flops), bytes_accessed=int(moved), transcendentals=0)


def params():
    return pltpu.CompilerParams(vmem_limit_bytes=VMEM_LIMIT)


def anywhere():
    return pl.BlockSpec(memory_space=pl.ANY)


def position():
    me = lax.axis_index("pts")
    chip = lax.div(me, 2)
    return me, chip, me - 2 * chip


def orbit_kernel(occupied, own_ref, mate_ref, w_ref, trial_any, orbit_ref, near_ref, sent_ref, trial_ref, sems):
    me, _, parity = position()
    copies = [
        pltpu.make_async_copy(trial_any.at[device], trial_ref.at[k], sems.at[k])
        for k, device in enumerate((me, me + 1 - 2 * parity))
    ]
    for copy in copies:
        copy.start()
    rows = own_ref.shape[0]
    x = jnp.concatenate([own_ref[...].astype(F32), mate_ref[...].astype(F32)], axis=0).astype(BF16)
    for copy in copies:
        copy.wait()
    trial = trial_ref[0].astype(F32)
    near = jnp.concatenate([trial, trial_ref[1].astype(F32)], axis=0)
    near_ref[...] = near.astype(BF16)
    lane = lax.broadcasted_iota(jnp.int32, (rows, 128), 1)
    density = jnp.zeros((rows, 128), F32)
    for pair in range(w_ref.shape[0] // (2 * occupied)):
        both = mm(x, w_ref[pair * 2 * occupied : (pair + 1) * 2 * occupied], NT).astype(BF16)
        for half in range(2):
            one = both[:, half * occupied : (half + 1) * occupied]
            walker = 2 * pair + half
            orbit_ref[walker] = one
            total = jnp.sum(one.astype(F32)[:rows] * trial, axis=1, keepdims=True)
            density = jnp.where(lane == walker, total / math.sqrt(occupied), density)
    turned = density.T[: sent_ref.shape[1]].astype(BF16)
    for device in range(sent_ref.shape[0]):
        sent_ref[device] = turned


def orbit_call(own, mate, turned_walkers, trial_blocks):
    rows, orbitals = own.shape
    devices, _, occupied = trial_blocks.shape
    walkers = turned_walkers.shape[0] // occupied
    return pl.pallas_call(
        functools.partial(orbit_kernel, occupied),
        out_shape=(
            jax.ShapeDtypeStruct((walkers, 2 * rows, occupied), BF16),
            jax.ShapeDtypeStruct((2 * rows, occupied), BF16),
            jax.ShapeDtypeStruct((devices // 2, -(-walkers // 16) * 16, rows), BF16),
        ),
        in_specs=[vmem()] * 3 + [anywhere()],
        out_specs=(vmem(), vmem(), vmem()),
        scratch_shapes=[pltpu.VMEM((2, rows, occupied), BF16), pltpu.SemaphoreType.DMA((2,))],
        compiler_params=params(),
        cost_estimate=cost(4 * rows * orbitals * walkers * occupied, 6e6),
        name="orbit",
    )(own, mate, turned_walkers, trial_blocks)


def split_kernel(core_ref, out_ref):
    width = out_ref.shape[3]
    _, _, parity = position()
    for block in range(core_ref.shape[1] // width):
        slot = lax.rem(block % 2 + parity, 2)
        out_ref[slot, block // 2] = core_ref[:, block * width : (block + 1) * width]


def split_call(core, width):
    rows, columns = core.shape
    return pl.pallas_call(
        split_kernel,
        out_shape=jax.ShapeDtypeStruct((2, columns // width // 2, rows, width), BF16),
        in_specs=[vmem()],
        out_specs=vmem(),
        compiler_params=params(),
        cost_estimate=cost(1e6, 6e6),
        name="split",
    )(core)


def field_kernel(walkers, occupied, columns, mine_ref, theirs_ref, cores_ref, draws_ref, out_ref, hartree_ref):
    total = None
    for chip in range(cores_ref.shape[1]):
        for slot, density_ref in enumerate((mine_ref, theirs_ref)):
            piece = mm(density_ref[chip], cores_ref[slot, chip], NT)
            total = piece if total is None else total + piece
    mine = mine_ref[position()[1]].astype(F32)
    hartree_ref[...] = jnp.broadcast_to(jnp.sum(mine * total, axis=1, keepdims=True), hartree_ref.shape)
    field = FIELD_STEP * (node_lookup(draws_ref[...]) - FIELD_STEP * total[:walkers])
    for chip in range(out_ref.shape[0]):
        first = columns * chip // occupied
        out_ref[chip, 0:1] = field[first : first + 1]
        second = min(first + 1, walkers - 1)
        out_ref[chip, 1:2] = field[second : second + 1]


def field_call(mine, theirs, cores, draws, occupied, columns):
    chips, padded, rows = mine.shape
    walkers = draws.shape[0]
    return pl.pallas_call(
        functools.partial(field_kernel, walkers, occupied, columns),
        out_shape=(
            jax.ShapeDtypeStruct((chips, 2, rows), F32),
            jax.ShapeDtypeStruct((padded, 128), F32),
        ),
        in_specs=[vmem()] * 4,
        out_specs=(vmem(), vmem()),
        compiler_params=params(),
        cost_estimate=cost(4e9, 4e6),
        name="field",
    )(mine, theirs, cores, draws)


def exchange_kernel(
    occupied, weight, offset, x_ref, w_ref, orbit_ref, near_ref, before_ref, trial_any, cores_any,
    came_any, out_ref, core_ref, far_ref, forward_ref, backward_ref, trial_ref, half_ref, sems,
):
    _, chip, parity = position()
    chips = cores_any.shape[1]
    far = lax.rem(chip + (offset + chips), chips)
    copies = [
        pltpu.make_async_copy(trial_any.at[2 * far + parity], trial_ref, sems.at[0]),
        pltpu.make_async_copy(cores_any.at[0, far], half_ref.at[0], sems.at[1]),
        pltpu.make_async_copy(came_any.at[0, far], half_ref.at[1], sems.at[2]),
    ]
    for copy in copies:
        copy.start()
    x = x_ref[...]
    rows = x.shape[0]
    far_ref[...] = mm(w_ref[...], x, NT).astype(BF16)
    for copy in copies:
        copy.wait()
    core_ref[:rows] = half_ref[0].astype(F32)
    core_ref[rows:] = half_ref[1].astype(F32)
    far_trial = trial_ref[...]
    walkers = out_ref.shape[0]
    forward_ref[1] = jnp.zeros(core_ref.shape, F32)
    backward_ref[1] = jnp.zeros(core_ref.shape, F32)

    def gather(walker, slot):
        value = forward_ref[slot] * backward_ref[slot] * core_ref[...]
        total = jnp.sum(value.reshape(-1, 8, rows), axis=0)
        out_ref[walker] = before_ref[walker] + weight * total

    def spread(walker, slot):
        orbit_far = far_ref[pl.ds(pl.multiple_of(walker * occupied, occupied), occupied)]
        forward_ref[slot] = mm(orbit_ref[walker], far_trial, NT)
        backward_ref[slot] = mm(near_ref[...], orbit_far)

    def two(number, carry):
        gather(lax.rem(2 * number + walkers - 1, walkers), 1)
        spread(2 * number, 0)
        gather(2 * number, 0)
        spread(2 * number + 1, 1)
        return carry

    lax.fori_loop(0, walkers // 2, two, 0)
    gather(walkers - 1, 1)


def exchange_call(offset, block, turned_walkers, orbit, near, trial_blocks, cores, came, before, weight):
    walkers, near_rows, occupied = orbit.shape
    rows = came.shape[2]
    orbitals = turned_walkers.shape[1]
    return pl.pallas_call(
        functools.partial(exchange_kernel, occupied, weight, offset),
        out_shape=jax.ShapeDtypeStruct(before.shape, F32),
        in_specs=[vmem()] * 5 + [anywhere()] * 3,
        out_specs=vmem(),
        scratch_shapes=[
            pltpu.VMEM((near_rows, rows), F32),
            pltpu.VMEM((walkers * occupied, rows), BF16),
            pltpu.VMEM((2, near_rows, rows), F32),
            pltpu.VMEM((2, near_rows, rows), F32),
            pltpu.VMEM((rows, occupied), BF16),
            pltpu.VMEM((2, rows, rows), BF16),
            pltpu.SemaphoreType.DMA((3,)),
        ],
        compiler_params=params(),
        cost_estimate=cost(2 * rows * walkers * occupied * (orbitals + 4 * rows), 5e6),
        name="exchange",
    )(block, turned_walkers, orbit, near, before, trial_blocks, cores, came)


def energy_row(walkers, occupied, shift, partial_ref, hartree_ref, points):
    exchange = jnp.sum(jnp.sum(partial_ref[...], axis=1), axis=1, keepdims=True) / occupied
    energy = (hartree_ref[:walkers] - exchange) / (2.0 * points)
    row = lax.broadcasted_iota(jnp.int32, energy.shape, 0)
    lane = lax.broadcasted_iota(jnp.int32, energy.shape, 1)
    return jnp.sum(jnp.where(lane == row + shift, energy, 0.0), axis=0, keepdims=True)


def step_term(degree, own_ref, other_ref, running_ref):
    columns = running_ref.shape[0]
    term = ((own_ref[:columns] + other_ref[:columns]) / degree).astype(BF16)
    return term, running_ref[...] + term.astype(F32)


def degree_kernel(offsets, degree, occupied, field_ref, *refs):
    count = len(offsets)
    _, chip, _ = position()
    blocks, refs = refs[:count], refs[count:]
    if degree == 1:
        walkers_any, partial_ref, hartree_ref, out_ref, running_ref, walkers_ref, sem = refs
        columns = walkers_ref.shape[0]
        start = pl.multiple_of(chip * columns, math.gcd(columns, 32))
        copy = pltpu.make_async_copy(walkers_any.at[pl.ds(start, columns)], walkers_ref, sem)
        copy.start()
        copy.wait()
        term = walkers_ref[...]
        running_ref[...] = term.astype(F32)
        points = 2 * count * field_ref.shape[2]
        row = energy_row(partial_ref.shape[0], occupied, columns, partial_ref, hartree_ref, points)
        out_ref[columns:, :128] = jnp.broadcast_to(row, (8, 128))
    else:
        own_ref, other_ref, before_ref, out_ref, running_ref = refs
        columns = before_ref.shape[0]
        term, running = step_term(degree - 1, own_ref, other_ref, before_ref)
        running_ref[...] = running
    first = occupied - lax.rem(chip * columns, occupied)
    total = None
    for number in range(count):
        x = blocks[number][...]
        current = mm(term, x, NT).astype(BF16).astype(F32)
        field = field_ref[lax.rem(chip + (offsets[number] + count), count)]
        column = lax.broadcasted_iota(jnp.int32, current.shape, 0)
        scaled = jnp.where(column < first, field[0:1], field[1:2]) * current
        piece = mm(scaled.astype(BF16), x)
        total = piece if total is None else total + piece
    out_ref[:columns] = total


def degree_call(offsets, fields, blocks, degree, occupied, columns, *rest):
    count = len(blocks)
    rows, orbitals = fields.shape[2], blocks[0].shape[1]
    return pl.pallas_call(
        functools.partial(degree_kernel, tuple(offsets), degree, occupied),
        out_shape=(
            jax.ShapeDtypeStruct((columns + 8 if degree == 1 else columns, orbitals), F32),
            jax.ShapeDtypeStruct((columns, orbitals), F32),
        ),
        in_specs=[vmem()] * (1 + count)
        + [anywhere() if degree == 1 else vmem()]
        + [vmem()] * (len(rest) - 1),
        out_specs=(vmem(), vmem()),
        scratch_shapes=[pltpu.VMEM((columns, orbitals), BF16), pltpu.SemaphoreType.DMA(())]
        if degree == 1
        else [],
        compiler_params=params(),
        cost_estimate=cost(4 * rows * count * orbitals * columns, 6e6),
        name="degree",
    )(fields, *blocks, *rest)


def finish_kernel(own_ref, other_ref, before_ref, own_energy, other_energy, out_ref, turned_ref):
    columns, orbitals = before_ref.shape
    chips, own_rows, lanes = out_ref.shape
    _, _, parity = position()
    _, running = step_term(TAYLOR, own_ref, other_ref, before_ref)
    padded = jnp.concatenate([running, jnp.zeros((lanes - columns, orbitals), F32)], axis=0)
    turned_ref[...] = padded.T
    energy = own_energy[:, :lanes] + other_energy[:, :lanes]
    top = energy.astype(BF16).astype(F32)
    middle = (energy - top).astype(BF16).astype(F32)
    low = energy - top - middle
    row = lax.broadcasted_iota(jnp.int32, (own_rows, lanes), 0)
    lane = lax.broadcasted_iota(jnp.int32, (own_rows, lanes), 1)
    extra = jnp.where(row == 0, top[0:1], jnp.where(row == 1, middle[0:1], jnp.where(row == 2, low[0:1], 0.0)))
    for chip in range(chips):
        mine = turned_ref[pl.ds((2 * chip + parity) * own_rows, own_rows)]
        out_ref[chip] = jnp.where(lane < columns, mine, extra).astype(BF16)


def finish_call(own, other, running, own_energy, other_energy, devices):
    columns, orbitals = running.shape
    return pl.pallas_call(
        finish_kernel,
        out_shape=jax.ShapeDtypeStruct((devices // 2, orbitals // devices, 128), BF16),
        in_specs=[vmem()] * 5,
        out_specs=vmem(),
        scratch_shapes=[pltpu.VMEM((orbitals, 128), F32)],
        compiler_params=params(),
        cost_estimate=cost(1e6, 2e6),
        name="finish",
    )(own, other, running, own_energy, other_energy)


def body(points_map, trial, core, walkers, draws):
    rows, orbitals = points_map.shape
    walker_count, occupied = walkers.shape[1:]
    devices = lax.axis_size("pts")
    chips = devices // 2
    swapped = [(i, i ^ 1) for i in range(devices)]
    forward = [(i, (i + 2) % devices) for i in range(devices)]
    backward = [(i, (i - 2) % devices) for i in range(devices)]
    same_core = [[2 * z + c for z in range(chips)] for c in range(2)]
    columns = walker_count * occupied // chips

    def swap(value):
        return lax.ppermute(value, "pts", swapped)

    def advance(right, left):
        return lax.ppermute(right, "pts", forward), lax.ppermute(left, "pts", backward)

    mate = swap(points_map)
    rights, lefts = [points_map], [points_map]
    for value, found in zip(advance(points_map, points_map), (rights, lefts)):
        found.append(value)
    turned = walkers.reshape(orbitals, walker_count * occupied).T
    trial_blocks = trial.reshape(devices, rows, occupied)
    orbit, near, sent = orbit_call(points_map, mate, turned, trial_blocks)
    sent, rights[1], lefts[1] = lax.optimization_barrier((sent, rights[1], lefts[1]))
    for value, found in zip(advance(rights[1], lefts[1]), (rights, lefts)):
        found.append(value)
    mine = lax.all_to_all(
        sent, "pts", split_axis=0, concat_axis=0, tiled=True, axis_index_groups=same_core
    )
    theirs = swap(mine)
    mine, rights[2], lefts[2] = lax.optimization_barrier((mine, rights[2], lefts[2]))
    for value, found in zip(advance(rights[2], lefts[2]), (rights, lefts)):
        found.append(value)
    cores = split_call(core, rows)
    came = swap(cores[1:2])
    outgoing, hartree = field_call(mine, theirs, cores, draws.T, occupied, columns)
    fields = lax.all_to_all(
        outgoing, "pts", split_axis=0, concat_axis=0, tiled=True, axis_index_groups=same_core
    )

    def exchange(offset, block, before, weight):
        return exchange_call(
            offset, block, turned, orbit, near, trial_blocks, cores, came, before, weight
        )

    partial = jnp.zeros((walker_count, 8, rows), F32)
    partial, fields = lax.optimization_barrier((partial, fields))
    half = chips // 2
    partial, rights[3], lefts[3] = lax.optimization_barrier((partial, rights[3], lefts[3]))
    for value, found in zip(advance(rights[3], lefts[3]), (rights, lefts)):
        found.append(value)
    for step in range(half + 1):
        right, left = rights[-1], lefts[-1]
        if step % 2 and len(rights) <= half:
            right, partial = lax.optimization_barrier((right, partial))
            rights.append(lax.ppermute(right, "pts", forward))
        weight = 1.0 if step in (0, half) else 2.0
        partial = exchange(-step, rights[step], partial, weight)
        if step % 2 and len(lefts) < half:
            left, partial = lax.optimization_barrier((left, partial))
            lefts.append(lax.ppermute(left, "pts", backward))
    blocks = rights + lefts[1:]
    offsets = [-step for step in range(half + 1)] + list(range(1, half))

    mine, running = degree_call(
        offsets, fields, blocks, 1, occupied, columns, turned, partial, hartree
    )
    theirs = swap(mine)
    energies = (mine[columns:], theirs[columns:])
    for degree in range(2, TAYLOR + 1):
        mine, running = degree_call(
            offsets, fields, blocks, degree, occupied, columns, mine, theirs, running
        )
        theirs = swap(mine)
    message = finish_call(mine, theirs, running, *energies, devices)
    arrived = lax.all_to_all(
        message, "pts", split_axis=0, concat_axis=0, tiled=True, axis_index_groups=same_core
    )
    new_walkers = jnp.moveaxis(arrived[:, :, :columns], 0, 1)
    new_walkers = new_walkers.reshape(orbitals // devices, walker_count, occupied)
    energy = jnp.sum(arrived[:, :3, columns : columns + walker_count].astype(F32), axis=(0, 1))
    return (new_walkers, energy)


def solution(mesh):
    placed = (
        P(("mol", "pts"), None),
        P("mol", None),
        P(("mol", "pts"), None),
        P("mol", None, None),
        P(("mol", "pts"), None),
    )
    return jax.shard_map(
        body,
        mesh=mesh,
        in_specs=placed,
        out_specs=(P(("mol", "pts"), None, None), P("mol")),
        check_vma=False,
    )
```

```python
import functools
import math

import jax
import jax.numpy as jnp
from jax import lax
from jax.experimental import pallas as pl
from jax.experimental.pallas import tpu as pltpu
from jax.sharding import PartitionSpec as P

TAYLOR = 3
GAUSS_NODES = (-2.3344142, -0.7419637, 0.7419637, 2.3344142)
FIELD_STEP = 0.15
BF16, F32 = jnp.bfloat16, jnp.float32
NT = (((1,), (1,)), ((), ()))
NN = (((1,), (0,)), ((), ()))
VMEM_LIMIT = 24 * 1024 * 1024


def mm(a, b, dims=NN):
    return lax.dot_general(a, b, dims, preferred_element_type=F32)


def node_lookup(draws):
    values = jnp.zeros(draws.shape, F32)
    for number, node in enumerate(GAUSS_NODES):
        values = values + jnp.where(draws == number, node, 0.0).astype(F32)
    return values


def vmem():
    return pl.BlockSpec(memory_space=pltpu.VMEM)


def cost(flops, moved):
    return pl.CostEstimate(flops=int(flops), bytes_accessed=int(moved), transcendentals=0)


def params():
    return pltpu.CompilerParams(vmem_limit_bytes=VMEM_LIMIT)


def anywhere():
    return pl.BlockSpec(memory_space=pl.ANY)


def position():
    me = lax.axis_index("pts")
    chip = lax.div(me, 2)
    return me, chip, me - 2 * chip


def orbit_kernel(occupied, own_ref, mate_ref, w_ref, trial_any, orbit_ref, near_ref, sent_ref, trial_ref, sems):
    me, _, parity = position()
    copies = [
        pltpu.make_async_copy(trial_any.at[device], trial_ref.at[k], sems.at[k])
        for k, device in enumerate((me, me + 1 - 2 * parity))
    ]
    for copy in copies:
        copy.start()
    rows = own_ref.shape[0]
    x = jnp.concatenate([own_ref[...].astype(F32), mate_ref[...].astype(F32)], axis=0).astype(BF16)
    for copy in copies:
        copy.wait()
    trial = trial_ref[0].astype(F32)
    near = jnp.concatenate([trial, trial_ref[1].astype(F32)], axis=0)
    near_ref[...] = near.astype(BF16)
    lane = lax.broadcasted_iota(jnp.int32, (rows, 128), 1)
    density = jnp.zeros((rows, 128), F32)
    for pair in range(w_ref.shape[0] // (2 * occupied)):
        both = mm(x, w_ref[pair * 2 * occupied : (pair + 1) * 2 * occupied], NT).astype(BF16)
        for half in range(2):
            one = both[:, half * occupied : (half + 1) * occupied]
            walker = 2 * pair + half
            orbit_ref[walker] = one
            total = jnp.sum(one.astype(F32)[:rows] * trial, axis=1, keepdims=True)
            density = jnp.where(lane == walker, total / math.sqrt(occupied), density)
    turned = density.T[: sent_ref.shape[1]].astype(BF16)
    for device in range(sent_ref.shape[0]):
        sent_ref[device] = turned


def orbit_call(own, mate, turned_walkers, trial_blocks):
    rows, orbitals = own.shape
    devices, _, occupied = trial_blocks.shape
    walkers = turned_walkers.shape[0] // occupied
    return pl.pallas_call(
        functools.partial(orbit_kernel, occupied),
        out_shape=(
            jax.ShapeDtypeStruct((walkers, 2 * rows, occupied), BF16),
            jax.ShapeDtypeStruct((2 * rows, occupied), BF16),
            jax.ShapeDtypeStruct((devices // 2, -(-walkers // 16) * 16, rows), BF16),
        ),
        in_specs=[vmem()] * 3 + [anywhere()],
        out_specs=(vmem(), vmem(), vmem()),
        scratch_shapes=[pltpu.VMEM((2, rows, occupied), BF16), pltpu.SemaphoreType.DMA((2,))],
        compiler_params=params(),
        cost_estimate=cost(4 * rows * orbitals * walkers * occupied, 6e6),
        name="orbit",
    )(own, mate, turned_walkers, trial_blocks)


def split_kernel(core_ref, out_ref):
    width = out_ref.shape[3]
    _, _, parity = position()
    for block in range(core_ref.shape[1] // width):
        slot = lax.rem(block % 2 + parity, 2)
        out_ref[slot, block // 2] = core_ref[:, block * width : (block + 1) * width]


def split_call(core, width):
    rows, columns = core.shape
    return pl.pallas_call(
        split_kernel,
        out_shape=jax.ShapeDtypeStruct((2, columns // width // 2, rows, width), BF16),
        in_specs=[vmem()],
        out_specs=vmem(),
        compiler_params=params(),
        cost_estimate=cost(1e6, 6e6),
        name="split",
    )(core)


def field_kernel(walkers, occupied, columns, mine_ref, theirs_ref, cores_ref, draws_ref, out_ref, hartree_ref):
    total = None
    for chip in range(cores_ref.shape[1]):
        for slot, density_ref in enumerate((mine_ref, theirs_ref)):
            piece = mm(density_ref[chip], cores_ref[slot, chip], NT)
            total = piece if total is None else total + piece
    mine = mine_ref[position()[1]].astype(F32)
    hartree_ref[...] = jnp.broadcast_to(jnp.sum(mine * total, axis=1, keepdims=True), hartree_ref.shape)
    field = FIELD_STEP * (node_lookup(draws_ref[...]) - FIELD_STEP * total[:walkers])
    for chip in range(out_ref.shape[0]):
        first = columns * chip // occupied
        out_ref[chip, 0:1] = field[first : first + 1]
        second = min(first + 1, walkers - 1)
        out_ref[chip, 1:2] = field[second : second + 1]


def field_call(mine, theirs, cores, draws, occupied, columns):
    chips, padded, rows = mine.shape
    walkers = draws.shape[0]
    return pl.pallas_call(
        functools.partial(field_kernel, walkers, occupied, columns),
        out_shape=(
            jax.ShapeDtypeStruct((chips, 2, rows), F32),
            jax.ShapeDtypeStruct((padded, 128), F32),
        ),
        in_specs=[vmem()] * 4,
        out_specs=(vmem(), vmem()),
        compiler_params=params(),
        cost_estimate=cost(4e9, 4e6),
        name="field",
    )(mine, theirs, cores, draws)


def exchange_kernel(
    occupied, weight, offset, x_ref, w_ref, orbit_ref, near_ref, before_ref, trial_any, cores_any,
    came_any, out_ref, core_ref, far_ref, forward_ref, backward_ref, trial_ref, half_ref, sems,
):
    _, chip, parity = position()
    chips = cores_any.shape[1]
    far = lax.rem(chip + (offset + chips), chips)
    copies = [
        pltpu.make_async_copy(trial_any.at[2 * far + parity], trial_ref, sems.at[0]),
        pltpu.make_async_copy(cores_any.at[0, far], half_ref.at[0], sems.at[1]),
        pltpu.make_async_copy(came_any.at[0, far], half_ref.at[1], sems.at[2]),
    ]
    for copy in copies:
        copy.start()
    x = x_ref[...]
    rows = x.shape[0]
    far_ref[...] = mm(w_ref[...], x, NT).astype(BF16)
    for copy in copies:
        copy.wait()
    core_ref[:rows] = half_ref[0].astype(F32)
    core_ref[rows:] = half_ref[1].astype(F32)
    far_trial = trial_ref[...]
    walkers = out_ref.shape[0]
    forward_ref[1] = jnp.zeros(core_ref.shape, F32)
    backward_ref[1] = jnp.zeros(core_ref.shape, F32)

    def gather(walker, slot):
        value = forward_ref[slot] * backward_ref[slot] * core_ref[...]
        total = jnp.sum(value.reshape(-1, 8, rows), axis=0)
        out_ref[walker] = before_ref[walker] + weight * total

    def spread(walker, slot):
        orbit_far = far_ref[pl.ds(pl.multiple_of(walker * occupied, occupied), occupied)]
        forward_ref[slot] = mm(orbit_ref[walker], far_trial, NT)
        backward_ref[slot] = mm(near_ref[...], orbit_far)

    def two(number, carry):
        gather(lax.rem(2 * number + walkers - 1, walkers), 1)
        spread(2 * number, 0)
        gather(2 * number, 0)
        spread(2 * number + 1, 1)
        return carry

    lax.fori_loop(0, walkers // 2, two, 0)
    gather(walkers - 1, 1)


def exchange_call(offset, block, turned_walkers, orbit, near, trial_blocks, cores, came, before, weight):
    walkers, near_rows, occupied = orbit.shape
    rows = came.shape[2]
    orbitals = turned_walkers.shape[1]
    return pl.pallas_call(
        functools.partial(exchange_kernel, occupied, weight, offset),
        out_shape=jax.ShapeDtypeStruct(before.shape, F32),
        in_specs=[vmem()] * 5 + [anywhere()] * 3,
        out_specs=vmem(),
        scratch_shapes=[
            pltpu.VMEM((near_rows, rows), F32),
            pltpu.VMEM((walkers * occupied, rows), BF16),
            pltpu.VMEM((2, near_rows, rows), F32),
            pltpu.VMEM((2, near_rows, rows), F32),
            pltpu.VMEM((rows, occupied), BF16),
            pltpu.VMEM((2, rows, rows), BF16),
            pltpu.SemaphoreType.DMA((3,)),
        ],
        compiler_params=params(),
        cost_estimate=cost(2 * rows * walkers * occupied * (orbitals + 4 * rows), 5e6),
        name="exchange",
    )(block, turned_walkers, orbit, near, before, trial_blocks, cores, came)


def energy_row(walkers, occupied, shift, partial_ref, hartree_ref, points):
    exchange = jnp.sum(jnp.sum(partial_ref[...], axis=1), axis=1, keepdims=True) / occupied
    energy = (hartree_ref[:walkers] - exchange) / (2.0 * points)
    row = lax.broadcasted_iota(jnp.int32, energy.shape, 0)
    lane = lax.broadcasted_iota(jnp.int32, energy.shape, 1)
    return jnp.sum(jnp.where(lane == row + shift, energy, 0.0), axis=0, keepdims=True)


def step_term(degree, own_ref, other_ref, running_ref):
    columns = running_ref.shape[0]
    term = ((own_ref[:columns] + other_ref[:columns]) / degree).astype(BF16)
    return term, running_ref[...] + term.astype(F32)


def degree_kernel(offsets, degree, occupied, field_ref, *refs):
    count = len(offsets)
    _, chip, _ = position()
    blocks, refs = refs[:count], refs[count:]
    if degree == 1:
        walkers_any, partial_ref, hartree_ref, out_ref, running_ref, walkers_ref, sem = refs
        columns = walkers_ref.shape[0]
        start = pl.multiple_of(chip * columns, math.gcd(columns, 32))
        copy = pltpu.make_async_copy(walkers_any.at[pl.ds(start, columns)], walkers_ref, sem)
        copy.start()
        copy.wait()
        term = walkers_ref[...]
        running_ref[...] = term.astype(F32)
        points = 2 * count * field_ref.shape[2]
        row = energy_row(partial_ref.shape[0], occupied, columns, partial_ref, hartree_ref, points)
        out_ref[columns:, :128] = jnp.broadcast_to(row, (8, 128))
    else:
        own_ref, other_ref, before_ref, out_ref, running_ref = refs
        columns = before_ref.shape[0]
        term, running = step_term(degree - 1, own_ref, other_ref, before_ref)
        running_ref[...] = running
    first = occupied - lax.rem(chip * columns, occupied)
    total = None
    for number in range(count):
        x = blocks[number][...]
        current = mm(term, x, NT).astype(BF16).astype(F32)
        field = field_ref[lax.rem(chip + (offsets[number] + count), count)]
        column = lax.broadcasted_iota(jnp.int32, current.shape, 0)
        scaled = jnp.where(column < first, field[0:1], field[1:2]) * current
        piece = mm(scaled.astype(BF16), x)
        total = piece if total is None else total + piece
    out_ref[:columns] = total


def degree_call(offsets, fields, blocks, degree, occupied, columns, *rest):
    count = len(blocks)
    rows, orbitals = fields.shape[2], blocks[0].shape[1]
    return pl.pallas_call(
        functools.partial(degree_kernel, tuple(offsets), degree, occupied),
        out_shape=(
            jax.ShapeDtypeStruct((columns + 8 if degree == 1 else columns, orbitals), F32),
            jax.ShapeDtypeStruct((columns, orbitals), F32),
        ),
        in_specs=[vmem()] * (1 + count)
        + [anywhere() if degree == 1 else vmem()]
        + [vmem()] * (len(rest) - 1),
        out_specs=(vmem(), vmem()),
        scratch_shapes=[pltpu.VMEM((columns, orbitals), BF16), pltpu.SemaphoreType.DMA(())]
        if degree == 1
        else [],
        compiler_params=params(),
        cost_estimate=cost(4 * rows * count * orbitals * columns, 6e6),
        name="degree",
    )(fields, *blocks, *rest)


def finish_kernel(own_ref, other_ref, before_ref, own_energy, other_energy, out_ref, turned_ref):
    columns, orbitals = before_ref.shape
    chips, own_rows, lanes = out_ref.shape
    _, _, parity = position()
    _, running = step_term(TAYLOR, own_ref, other_ref, before_ref)
    padded = jnp.concatenate([running, jnp.zeros((lanes - columns, orbitals), F32)], axis=0)
    turned_ref[...] = padded.T
    energy = own_energy[:, :lanes] + other_energy[:, :lanes]
    top = energy.astype(BF16).astype(F32)
    middle = (energy - top).astype(BF16).astype(F32)
    low = energy - top - middle
    row = lax.broadcasted_iota(jnp.int32, (own_rows, lanes), 0)
    lane = lax.broadcasted_iota(jnp.int32, (own_rows, lanes), 1)
    extra = jnp.where(row == 0, top[0:1], jnp.where(row == 1, middle[0:1], jnp.where(row == 2, low[0:1], 0.0)))
    for chip in range(chips):
        mine = turned_ref[pl.ds((2 * chip + parity) * own_rows, own_rows)]
        out_ref[chip] = jnp.where(lane < columns, mine, extra).astype(BF16)


def finish_call(own, other, running, own_energy, other_energy, devices):
    columns, orbitals = running.shape
    return pl.pallas_call(
        finish_kernel,
        out_shape=jax.ShapeDtypeStruct((devices // 2, orbitals // devices, 128), BF16),
        in_specs=[vmem()] * 5,
        out_specs=vmem(),
        scratch_shapes=[pltpu.VMEM((orbitals, 128), F32)],
        compiler_params=params(),
        cost_estimate=cost(1e6, 2e6),
        name="finish",
    )(own, other, running, own_energy, other_energy)


def body(points_map, trial, core, walkers, draws):
    rows, orbitals = points_map.shape
    walker_count, occupied = walkers.shape[1:]
    devices = lax.axis_size("pts")
    chips = devices // 2
    swapped = [(i, i ^ 1) for i in range(devices)]
    forward = [(i, (i + 2) % devices) for i in range(devices)]
    backward = [(i, (i - 2) % devices) for i in range(devices)]
    same_core = [[2 * z + c for z in range(chips)] for c in range(2)]
    columns = walker_count * occupied // chips

    def swap(value):
        return lax.ppermute(value, "pts", swapped)

    def advance(right, left):
        return lax.ppermute(right, "pts", forward), lax.ppermute(left, "pts", backward)

    mate = swap(points_map)
    rights, lefts = [points_map], [points_map]
    for value, found in zip(advance(points_map, points_map), (rights, lefts)):
        found.append(value)
    cores = split_call(core, rows)
    came = swap(cores[1:2])
    walkers, cores, rights[1], lefts[1] = lax.optimization_barrier(
        (walkers, cores, rights[1], lefts[1])
    )
    for value, found in zip(advance(rights[1], lefts[1]), (rights, lefts)):
        found.append(value)
    turned = walkers.reshape(orbitals, walker_count * occupied).T
    trial_blocks = trial.reshape(devices, rows, occupied)
    orbit, near, sent = orbit_call(points_map, mate, turned, trial_blocks)
    sent, rights[2], lefts[2] = lax.optimization_barrier((sent, rights[2], lefts[2]))
    mine = lax.all_to_all(
        sent, "pts", split_axis=0, concat_axis=0, tiled=True, axis_index_groups=same_core
    )
    theirs = swap(mine)
    for value, found in zip(advance(rights[2], lefts[2]), (rights, lefts)):
        found.append(value)
    outgoing, hartree = field_call(mine, theirs, cores, draws.T, occupied, columns)
    fields = lax.all_to_all(
        outgoing, "pts", split_axis=0, concat_axis=0, tiled=True, axis_index_groups=same_core
    )

    def exchange(offset, block, before, weight):
        return exchange_call(
            offset, block, turned, orbit, near, trial_blocks, cores, came, before, weight
        )

    partial = jnp.zeros((walker_count, 8, rows), F32)
    partial, fields = lax.optimization_barrier((partial, fields))
    half = chips // 2
    partial, rights[3], lefts[3] = lax.optimization_barrier((partial, rights[3], lefts[3]))
    for value, found in zip(advance(rights[3], lefts[3]), (rights, lefts)):
        found.append(value)
    for step in range(half + 1):
        right, left = rights[-1], lefts[-1]
        if step % 2 and len(rights) <= half:
            right, partial = lax.optimization_barrier((right, partial))
            rights.append(lax.ppermute(right, "pts", forward))
        weight = 1.0 if step in (0, half) else 2.0
        partial = exchange(-step, rights[step], partial, weight)
        if step % 2 and len(lefts) < half:
            left, partial = lax.optimization_barrier((left, partial))
            lefts.append(lax.ppermute(left, "pts", backward))
    blocks = rights + lefts[1:]
    offsets = [-step for step in range(half + 1)] + list(range(1, half))

    mine, running = degree_call(
        offsets, fields, blocks, 1, occupied, columns, turned, partial, hartree
    )
    theirs = swap(mine)
    energies = (mine[columns:], theirs[columns:])
    for degree in range(2, TAYLOR + 1):
        mine, running = degree_call(
            offsets, fields, blocks, degree, occupied, columns, mine, theirs, running
        )
        theirs = swap(mine)
    message = finish_call(mine, theirs, running, *energies, devices)
    arrived = lax.all_to_all(
        message, "pts", split_axis=0, concat_axis=0, tiled=True, axis_index_groups=same_core
    )
    new_walkers = jnp.moveaxis(arrived[:, :, :columns], 0, 1)
    new_walkers = new_walkers.reshape(orbitals // devices, walker_count, occupied)
    energy = jnp.sum(arrived[:, :3, columns : columns + walker_count].astype(F32), axis=(0, 1))
    return (new_walkers, energy)


def solution(mesh):
    placed = (
        P(("mol", "pts"), None),
        P("mol", None),
        P(("mol", "pts"), None),
        P("mol", None, None),
        P(("mol", "pts"), None),
    )
    return jax.shard_map(
        body,
        mesh=mesh,
        in_specs=placed,
        out_specs=(P(("mol", "pts"), None, None), P("mol")),
        check_vma=False,
    )
```
